32 devices in a mesh: win: 4 (over y, core), tile: 8 (over z, x).
Axes of the slice: x: 2, y: 2, z: 4, core: 2. Of those that a mesh axis runs over, the one named last changes fastest.
Arguments:
- state: float32 [4, 8, 5, 32, 8, 128], P('win', 'tile'), may hold values from -6 to 6
- obs_weight: float32 [4, 8, 5, 32, 8, 128], P('win', 'tile'), may hold values from 0 to 1
- trajectory: bfloat16 [4, 8, 3, 2, 32, 8, 128], P('win', 'tile'), may hold values from -0.8984375 to 0.8984375
- coupling: float32 [5, 5], replicated, may hold values from -0.9 to 0.9
- prec_scale: float32 [5, 32], replicated, may hold values from 0.5 to 2
Outputs:
- hess_vec: float32 [4, 8, 5, 32, 8, 128], P('win', 'tile')
The draws below stay inside these ranges and needn't reach their ends.
All inputs are finite; a program needn't handle non-finite values.
Results may differ from the reference program's by a relative error of at most 0.0003.
Values sent between devices are 32-bit elements; how exact they have to be, the bound alone decides.
A program may use at most 64 MiB of HBM per device.

```python
import math
import jax
import jax.numpy as jnp
from jax import lax

VARS = 5
LEVELS = 32
STEPS = 3
TY = 4
CX = 8
CY = 128
WINDOWS = 4
TILES = 8
XTILES = 2


def shard_levels(stream_key, dims, shards, low, top_value):
    def one(axis_at, blocks):
        heights = jax.random.uniform(jax.random.fold_in(jax.random.fold_in(stream_key, 6), axis_at), (blocks,), jnp.float32, low / len(shards), top_value / len(shards))
        return jnp.repeat(jnp.exp(heights), dims[axis_at] // blocks).reshape((-1,) + (1,) * (len(dims) - axis_at - 1))

    gain = one(*shards[0])
    for cut in shards[1:]:
        gain = gain * one(*cut)
    return gain


def bell_draw(stream_key, extent, scale, most, pieces=(), dtype=jnp.bfloat16):
    array = scale * jax.random.normal(stream_key, extent, jnp.float32)
    if pieces:
        array = array * shard_levels(stream_key, extent, pieces, -0.22, 0.18)
    return jnp.clip(array, -most, most).astype(dtype)


def setup_inputs(seed: int = 0) -> dict:
    streams_of = jax.random.split(jax.random.key(seed), 6)
    return {
        "state": bell_draw(streams_of[0], (WINDOWS, TILES, VARS, LEVELS, CX, CY), 1.0, 6.0, ((0, 4), (1, 8)), jnp.float32),
        "obs_weight": jnp.clip(1.0 * jax.random.uniform(streams_of[1], (WINDOWS, TILES, VARS, LEVELS, CX, CY), jnp.float32) ** shard_levels(streams_of[1], (WINDOWS, TILES, VARS, LEVELS, CX, CY), ((0, 4), (1, 8)), -0.2, 0.2), 0.0, 1.0),
        "trajectory": bell_draw(streams_of[2], (WINDOWS, TILES, STEPS, 2, LEVELS, CX, CY), 0.15, 0.8984375, ((0, 4), (1, 8))),
        "coupling": bell_draw(streams_of[3], (VARS, VARS), 0.15, 0.9, (), jnp.float32),
        "prec_scale": jnp.clip(jnp.exp(jax.random.uniform(streams_of[4], (VARS, LEVELS), jnp.float32, math.log(0.5), math.log(2.0))), 0.5, 2.0),
    }


smooth_weight = 0.2


def to_grid(blocks):
    leading = blocks.shape[1:-2]
    blocks = blocks.reshape((XTILES, TY) + leading + (CX, CY))
    blocks = jnp.moveaxis(blocks, 0, -3)
    blocks = jnp.moveaxis(blocks, 0, -2)
    return blocks.reshape(leading + (XTILES * CX, TY * CY))


def from_grid(field):
    leading = field.shape[:-2]
    field = field.reshape(leading + (XTILES, CX, TY, CY))
    field = jnp.moveaxis(field, -2, 0)
    field = jnp.moveaxis(field, -3, 0)
    return field.reshape((TILES,) + leading + (CX, CY))


def beside(field_x, field_y):
    east_side = jnp.roll(field_x, -1, axis=-2)
    west_side = jnp.roll(field_x, 1, axis=-2)
    north_edge = jnp.roll(field_y[..., :1], -CX, axis=-2)
    south_edge = jnp.roll(field_y[..., -1:], CX, axis=-2)
    north_side = jnp.concatenate([field_y[..., 1:], north_edge], axis=-1)
    south_side = jnp.concatenate([south_edge, field_y[..., :-1]], axis=-1)
    return east_side, west_side, north_side, south_side


def tangent(field, winds, coupling):
    east_side, west_side, north_side, south_side = beside(field, field)
    mixed = jnp.einsum("vw,wlxy->vlxy", coupling, field, precision=lax.Precision.HIGHEST)
    return field + winds[0] * (east_side - west_side) + winds[1] * (north_side - south_side) + mixed


def adjoint(cotangent, winds, coupling):
    east_side, west_side, north_side, south_side = beside(winds[0] * cotangent, winds[1] * cotangent)
    mixed = jnp.einsum("wv,wlxy->vlxy", coupling, cotangent, precision=lax.Precision.HIGHEST)
    return cotangent + (west_side - east_side) + (south_side - north_side) + mixed


def precision_apply(field, prec_scale):
    east_side, west_side, north_side, south_side = beside(field, field)
    stencil = (1.0 + 4.0 * smooth_weight) * field - smooth_weight * (east_side + west_side + north_side + south_side)
    return prec_scale[:, :, None, None] * stencil


def reference(state, obs_weight, trajectory, coupling, prec_scale):
    states = [to_grid(state[window]) for window in range(WINDOWS)]
    moved = []
    for window in range(WINDOWS):
        winds_all = to_grid(trajectory[window])
        field = states[window]
        for step_number in range(STEPS):
            field = tangent(field, winds_all[step_number].astype(jnp.float32), coupling)
        moved.append(field)
    weighted = []
    for window in range(WINDOWS):
        if window == 0:
            mismatch = states[0]
        else:
            mismatch = states[window] - moved[window - 1]
        weighted.append(precision_apply(mismatch, prec_scale))
    outputs = []
    for window in range(WINDOWS):
        result = weighted[window] + to_grid(obs_weight[window]) * states[window]
        if window + 1 < WINDOWS:
            winds_all = to_grid(trajectory[window])
            cotangent = weighted[window + 1]
            for step_number in reversed(range(STEPS)):
                cotangent = adjoint(cotangent, winds_all[step_number].astype(jnp.float32), coupling)
            result = result - cotangent
        outputs.append(from_grid(result))
    return jnp.stack(outputs)
```

```python
import functools

import jax
import jax.numpy as jnp
from jax import lax
from jax.experimental import pallas as pl
from jax.experimental.pallas import tpu as pltpu
from jax.sharding import PartitionSpec as P

TY = 4
GROUP = 8

smooth_weight = 0.2


def kernel(windows, tiles, keep, state, obs, winds, coupling, prec, out,
           nat, onat, wnat, cs, ps, fld, wr, arrived, wgt, gf, ret, xs, xr, ys, yr,
           load, hsend, hrecv, wsend, wrecv, msend, mrecv):
    steps, groups, cx, cy = wr.shape[0] // 2, wr.shape[1], wr.shape[2], wr.shape[4]
    variables = fld.shape[1]
    span = GROUP * cx
    end = windows - 1
    moved, edge, back0 = steps, steps + 1, steps + 2
    helping = keep < groups
    k = lax.axis_index("win")
    t = lax.axis_index("tile")
    before_x, after_x = lax.rem(t + tiles - TY, tiles), lax.rem(t + TY, tiles)
    before_y, after_y = lax.rem(t + tiles - 1, tiles), lax.rem(t + 1, tiles)
    around = (before_x, after_x, before_y, after_y)
    is_first, is_last = k == 0, k == end
    lo, hi = jnp.where(is_last, keep, 0), jnp.where(is_first, keep, groups)
    sel = jnp.where(is_last, 1, 0)
    nxt = jnp.where(is_last, 1, k + 1)
    edges = jnp.where(is_last, edge, 0)

    def when(cond):
        return pl.when(cond)

    def part(g):
        return pl.ds(pl.multiple_of(g * span, span), span)

    def state_in(g):
        return pltpu.make_async_copy(state.at[:, part(g)], nat.at[:, part(g)], load.at[g])

    def winds_in(n):
        return pltpu.make_async_copy(winds.at[pl.ds(2 * n, 2)], wnat.at[pl.ds(2 * n, 2)], load.at[groups + n])

    obs_in = pltpu.make_async_copy(obs, onat, load.at[groups + steps])
    prec_in = pltpu.make_async_copy(prec, ps, load.at[groups + steps + 1])
    coupling_in = pltpu.make_async_copy(coupling, cs, load.at[groups + steps + 2])

    order = tuple(range(keep, groups)) + tuple(range(keep))
    for g in order:
        state_in(g).start()
    coupling_in.start()

    @when(~is_last)
    def _():
        for n in range(steps):
            winds_in(n).start()
    prec_in.start()
    obs_in.start()

    barrier = pltpu.get_barrier_semaphore()

    def greet(win, others):
        pl.semaphore_signal(barrier, inc=1, device_id={"win": win})
        for other in others:
            pl.semaphore_signal(barrier, inc=1, device_id={"win": win, "tile": other})
        return

    for other in around:
        pl.semaphore_signal(barrier, inc=1, device_id={"tile": other})

    @when(k < end)
    def _():
        greet(k + 1, around)

    @when(k > 0)
    def _():
        greet(k - 1, around)

    met = 4 + 5 * jnp.where(k < end, 1, 0) + 5 * jnp.where(k > 0, 1, 0)
    if helping:
        @when(is_first)
        def _():
            greet(end, ())

        @when(k == 1)
        def _():
            greet(end, around)

        @when(is_last)
        def _():
            greet(0, ())
            greet(1, around)
        met = met + jnp.where(is_first, 1, 0) + 5 * jnp.where(k == 1, 1, 0) + 6 * jnp.where(is_last, 1, 0)

    shape = (GROUP, cy)
    lane = lax.broadcasted_iota(jnp.int32, shape, 1)
    level = lax.broadcasted_iota(jnp.int32, shape, 0)
    pair, odd = lane // 2, lane % 2 == 1
    at_start, at_end = lane == 0, lane == cy - 1

    def halo(slot, g, win, low, high):
        made = []
        for side, to in enumerate((before_y, after_y)):
            made.append(pltpu.make_async_remote_copy(
                src_ref=ys.at[slot, g], dst_ref=yr.at[slot, side, g],
                send_sem=hsend.at[slot, side, g], recv_sem=hrecv.at[slot, side, g],
                device_id={"win": win, "tile": to}))
        for side, (to, rows) in enumerate(((before_x, low), (after_x, high))):
            made.append(pltpu.make_async_remote_copy(
                src_ref=rows, dst_ref=xr.at[slot, side, g],
                send_sem=hsend.at[slot, 2 + side, g], recv_sem=hrecv.at[slot, 2 + side, g],
                device_id={"win": win, "tile": to}))
        return made

    def field_halo(slot, g, win, index):
        return halo(slot, g, win, fld.at[index, :, g, 0], fld.at[index, :, g, cx - 1])

    def flux_halo(slot, g):
        return halo(slot, g, k, xs.at[slot - back0, 0, g], xs.at[slot - back0, 1, g])

    def receive(slot, g):
        for copy in halo(slot, g, k, xr.at[slot, 0, g], xr.at[slot, 1, g]):
            copy.wait_recv()

    def onward(g):
        return pltpu.make_async_remote_copy(
            src_ref=fld.at[steps + 1, :, g], dst_ref=arrived.at[:, g],
            send_sem=wsend.at[0, g], recv_sem=wrecv.at[0, g], device_id={"win": nxt})

    def back(g):
        source = jnp.where(k == 1, jnp.where(g < keep, 0, end), k - 1)
        return pltpu.make_async_remote_copy(
            src_ref=wgt.at[0, :, g], dst_ref=gf.at[0, :, g],
            send_sem=wsend.at[1, g], recv_sem=wrecv.at[1, g], device_id={"win": source})

    def lend_state(g):
        return pltpu.make_async_remote_copy(
            src_ref=fld.at[0, :, g], dst_ref=fld.at[1, :, g],
            send_sem=msend.at[0, g], recv_sem=mrecv.at[0, g], device_id={"win": end})

    def lend_winds(n, g):
        return pltpu.make_async_remote_copy(
            src_ref=wr.at[pl.ds(2 * n, 2), g], dst_ref=wr.at[pl.ds(2 * n, 2), g],
            send_sem=msend.at[2 + n, g], recv_sem=mrecv.at[2 + n, g], device_id={"win": end})

    def give_back(g):
        return pltpu.make_async_remote_copy(
            src_ref=ret.at[:, g], dst_ref=ret.at[:, g],
            send_sem=msend.at[1, g], recv_sem=mrecv.at[1, g], device_id={"win": 0})

    def place(v, r):
        return v * cx + r

    def pack(packed, value, v, r):
        p = place(v, r)
        return jnp.where(pair == p, pltpu.roll(value, 2 * p + 1, 1), packed)

    def rims(north, south):
        return jnp.where(odd, north, pltpu.roll(south, 2, 1))

    def sides(value, rim, v, r):
        edge_pair = pltpu.roll(rim, cy - 2 - 2 * place(v, r), 1)
        north = jnp.where(at_end, edge_pair, pltpu.roll(value, cy - 1, 1))
        south = jnp.where(at_start, edge_pair, pltpu.roll(value, 1, 1))
        return north, south

    def every(f):
        for v in range(variables):
            f(v)

    def rows_of(g, r):
        return pl.ds(g * span + r, GROUP, stride=cx)

    def convert_state(g):
        for v in range(variables):
            for r in range(cx):
                fld[0, v, g, r] = nat[v, rows_of(g, r), :]

    def pack_state(g, index, slot):
        packed = jnp.zeros(shape, jnp.float32)
        for v in range(variables):
            for r in range(cx):
                packed = pack(packed, fld[index, v, g, r], v, r)
        ys[slot, g] = packed

    def over(a, b, f):
        lax.fori_loop(a, b, lambda g, c: (f(g), c)[1], 0)

    for g in order:
        state_in(g).wait()
        convert_state(g)
        if g == order[0]:
            pl.semaphore_wait(barrier, met)
        if g >= keep:
            @when(is_first)
            def _():
                lend_state(g).start()

        @when((k < end) & (g < hi))
        def _():
            pack_state(g, 0, 0)
            for copy in field_halo(0, g, k, 0):
                copy.start()

    def convert_winds(n, g):
        for way in range(2):
            for j in range(GROUP):
                tile = wnat[2 * n + way, g * GROUP + j].astype(jnp.float32)
                for r in range(cx):
                    wr[2 * n + way, g, r, pl.ds(j, 1), :] = tile[r:r + 1]

    @when(k < end)
    def _():
        for n in range(steps):
            winds_in(n).wait()

            def one(i, n=n):
                g = lax.rem(i + keep, groups)
                convert_winds(n, g)
                if helping:
                    @when(is_first & (g >= keep))
                    def _():
                        lend_winds(n, g).start()
            over(0, groups, one)

    coupling_in.wait()

    if helping:
        @when(is_last)
        def _():
            @functools.partial(over, keep, groups)
            def _(g):
                lend_state(g).wait_recv()
                pack_state(g, 1, 0)
                for copy in field_halo(0, g, k, 1):
                    copy.start()

    @when(is_last)
    def _():
        @functools.partial(over, 0, groups)
        def _(g):
            pack_state(g, 0, edge)
            for copy in field_halo(edge, g, k, 0):
                copy.start()

    def forward(n, g):
        if helping:
            @when(is_last)
            def _():
                lend_winds(n, g).wait_recv()
        receive(n, g)
        source = jnp.where(n == 0, sel, n + 1)
        rim = rims(yr[n, 0, g], yr[n, 1, g])

        def row(r):
            if r < 0:
                return [xr[n, 1, g, v] for v in range(variables)]
            if r == cx:
                return [xr[n, 0, g, v] for v in range(variables)]
            return [fld[source, v, g, r] for v in range(variables)]

        west, here = row(-1), row(0)
        packed = jnp.zeros(shape, jnp.float32)
        for r in range(cx):
            east = row(r + 1)
            u, w = wr[2 * n, g, r], wr[2 * n + 1, g, r]
            for v in range(variables):
                north, south = sides(here[v], rim, v, r)
                total = here[v] + u * (east[v] - west[v]) + w * (north - south)
                for b in range(variables):
                    total = total + cs[v, b] * here[b]
                fld[n + 2, v, g, r] = total
                packed = pack(packed, total, v, r)
            west, here = here, east
        ys[n + 1, g] = packed
        ends = n == steps - 1
        for copy in field_halo(n + 1, g, jnp.where(ends, nxt, k), n + 2):
            copy.start()

        @when(ends)
        def _():
            onward(g).start()

    @functools.partial(over, 0, steps)
    def _(n):
        over(lo, hi, lambda g: forward(n, g))

    prec_in.wait()

    def stencil(g, row, rim, index):
        scale = []
        for v in range(variables):
            s = jnp.zeros(shape, jnp.float32)
            for j in range(GROUP):
                s = jnp.where(level == j, ps[v, g * GROUP + j], s)
            scale.append(s)
        west, here = row(-1), row(0)
        for r in range(cx):
            east = row(r + 1)
            for v in range(variables):
                north, south = sides(here[v], rim, v, r)
                smooth = (1.0 + 4.0 * smooth_weight) * here[v] - smooth_weight * (
                    east[v] + west[v] + north + south)
                wgt[index, v, g, r] = scale[v] * smooth
            west, here = here, east

    def start_window(g):
        def row(r):
            if r < 0:
                return [xr[0, 1, g, v] for v in range(variables)]
            if r == cx:
                return [xr[0, 0, g, v] for v in range(variables)]
            return [fld[sel, v, g, r] for v in range(variables)]
        stencil(g, row, rims(yr[0, 0, g], yr[0, 1, g]), sel)

    def mismatch(g):
        @when(is_last)
        def _():
            receive(edge, g)
        receive(moved, g)
        onward(g).wait_recv()

        def row(r):
            if r < 0:
                return [xr[edges, 1, g, v] - xr[moved, 1, g, v] for v in range(variables)]
            if r == cx:
                return [xr[edges, 0, g, v] - xr[moved, 0, g, v] for v in range(variables)]
            return [fld[0, v, g, r] - arrived[v, g, r] for v in range(variables)]
        stencil(g, row, rims(yr[edges, 0, g] - yr[moved, 0, g], yr[edges, 1, g] - yr[moved, 1, g]), 0)
        back(g).start()

    @when(k > 0)
    def _():
        over(0, groups, mismatch)

    @when(is_first | is_last)
    def _():
        over(lo, hi, start_window)

    def begin_back(g):
        back(g).wait_recv()
        n = steps - 1
        packed = jnp.zeros(shape, jnp.float32)
        for r in range(cx):
            u, w = wr[2 * n, g, r], wr[2 * n + 1, g, r]
            for v in range(variables):
                value = gf[0, v, g, r]
                if r == 0:
                    xs[0, 0, g, v] = u * value
                if r == cx - 1:
                    xs[0, 1, g, v] = u * value
                packed = pack(packed, w * value, v, r)
        ys[back0, g] = packed
        for copy in flux_halo(back0, g):
            copy.start()

    def backward(i, g, final):
        n = steps - 1 - i
        slot = back0 + i
        receive(slot, g)
        rim = rims(yr[slot, 0, g], yr[slot, 1, g])

        def row(r):
            if r < 0:
                return None, [xr[slot, 1, g, v] for v in range(variables)]
            if r == cx:
                return None, [xr[slot, 0, g, v] for v in range(variables)]
            u = wr[2 * n, g, r]
            values = [gf[i, v, g, r] for v in range(variables)]
            return values, [u * value for value in values]

        (_, west), (values, here) = row(-1), row(0)
        packed = jnp.zeros(shape, jnp.float32)
        for r in range(cx):
            values_east, east = row(r + 1)
            w = wr[2 * n + 1, g, r]
            if not final:
                u_next, w_next = wr[2 * n - 2, g, r], wr[2 * n - 1, g, r]
            for v in range(variables):
                north, south = sides(w * values[v], rim, v, r)
                total = values[v] + (west[v] - east[v]) + (south - north)
                for b in range(variables):
                    total = total + cs[b, v] * values[b]
                if final:
                    ret[v, g, r] = wgt[sel, v, g, r] - total
                    continue
                gf[i + 1, v, g, r] = total
                if r == 0:
                    xs[i + 1, 0, g, v] = u_next * total
                if r == cx - 1:
                    xs[i + 1, 1, g, v] = u_next * total
                packed = pack(packed, w_next * total, v, r)
            west, values, here = here, values_east, east
        if not final:
            ys[slot + 1, g] = packed
            for copy in flux_halo(slot + 1, g):
                copy.start()

    over(lo, hi, begin_back)

    @functools.partial(over, 0, steps - 1)
    def _(i):
        over(lo, hi, lambda g: backward(i, g, False))

    obs_in.wait()

    def finish(g, term):
        for v in range(variables):
            for r in range(cx):
                rows = rows_of(g, r)
                out[v, rows, :] = term(v, g, r) + onat[v, rows, :] * fld[0, v, g, r]

    @functools.partial(over, lo, hi)
    def _(g):
        backward(steps - 1, g, True)

        @when(~is_last)
        def _():
            finish(g, lambda v, g, r: ret[v, g, r])
        if helping:
            @when(is_last)
            def _():
                give_back(g).start()

    @when(is_last)
    def _():
        @functools.partial(over, 0, groups)
        def _(g):
            finish(g, lambda v, g, r: wgt[0, v, g, r])

    if helping:
        @when(is_first)
        def _():
            @functools.partial(over, keep, groups)
            def _(g):
                give_back(g).wait_recv()
                finish(g, lambda v, g, r: ret[v, g, r])

    def sent(copies):
        for copy in copies:
            copy.wait_send()

    @functools.partial(over, lo, hi)
    def _(g):
        for n in range(steps + 1):
            sent(field_halo(n, g, k, 0))
        for i in range(steps):
            sent(flux_halo(back0 + i, g))
        onward(g).wait_send()

    @when(k > 0)
    def _():
        over(0, groups, lambda g: back(g).wait_send())

    @when(is_last)
    def _():
        over(0, groups, lambda g: sent(field_halo(edge, g, k, 0)))
        if helping:
            over(keep, groups, lambda g: give_back(g).wait_send())

    if helping:
        @when(is_first)
        def _():
            @functools.partial(over, keep, groups)
            def _(g):
                lend_state(g).wait_send()
                for n in range(steps):
                    lend_winds(n, g).wait_send()


def solution(mesh):
    windows, tiles = mesh.shape["win"], mesh.shape["tile"]

    def body(state, obs, trajectory, coupling, prec):
        block = state.shape[2:]
        variables, levels, cx, cy = block
        steps = trajectory.shape[2]
        groups = levels // GROUP
        keep = groups
        slots = 2 * steps + 2
        flat = (variables, levels * cx, cy)
        field = (variables, groups, cx, GROUP, cy)
        anywhere = pl.BlockSpec(memory_space=pltpu.HBM)
        f32 = jnp.float32
        result = pl.pallas_call(
            functools.partial(kernel, windows, tiles, keep),
            out_shape=jax.ShapeDtypeStruct(flat, f32),
            in_specs=[anywhere] * 5,
            out_specs=pl.BlockSpec(memory_space=pltpu.VMEM),
            scratch_shapes=[
                pltpu.VMEM(flat, f32),
                pltpu.VMEM(flat, f32),
                pltpu.VMEM((2 * steps, levels, cx, cy), trajectory.dtype),
                pltpu.SMEM(coupling.shape, f32),
                pltpu.SMEM(prec.shape, f32),
                pltpu.VMEM((steps + 2,) + field, f32),
                pltpu.VMEM((2 * steps, groups, cx, GROUP, cy), f32),
                pltpu.VMEM(field, f32),
                pltpu.VMEM((2,) + field, f32),
                pltpu.VMEM((steps,) + field, f32),
                pltpu.VMEM(field, f32),
                pltpu.VMEM((steps, 2, groups, variables, GROUP, cy), f32),
                pltpu.VMEM((slots, 2, groups, variables, GROUP, cy), f32),
                pltpu.VMEM((slots, groups, GROUP, cy), f32),
                pltpu.VMEM((slots, 2, groups, GROUP, cy), f32),
                pltpu.SemaphoreType.DMA((groups + steps + 3,)),
                pltpu.SemaphoreType.DMA((slots, 4, groups)),
                pltpu.SemaphoreType.DMA((slots, 4, groups)),
                pltpu.SemaphoreType.DMA((2, groups)),
                pltpu.SemaphoreType.DMA((2, groups)),
                pltpu.SemaphoreType.DMA((2 + steps, groups)),
                pltpu.SemaphoreType.DMA((2 + steps, groups)),
            ],
            compiler_params=pltpu.CompilerParams(
                collective_id=0, has_side_effects=True, vmem_limit_bytes=48 * 2**20),
        )(*[pltpu.with_memory_space_constraint(x, pltpu.HBM) for x in (
            state.reshape(flat), obs.reshape(flat),
            trajectory.reshape((2 * steps, levels, cx, cy)), coupling, prec)])
        return result.reshape((1, 1) + block)

    spec = P("win", "tile", None, None, None, None)
    return jax.shard_map(
        body, mesh=mesh,
        in_specs=(spec, spec, P("win", "tile", None, None, None, None, None), P(), P()),
        out_specs=spec, check_vma=False)
```

```python
import functools

import jax
import jax.numpy as jnp
from jax import lax
from jax.experimental import pallas as pl
from jax.experimental.pallas import tpu as pltpu
from jax.sharding import PartitionSpec as P

TY = 4
GROUP = 8

smooth_weight = 0.2


def kernel(windows, tiles, keep, state, obs, winds, coupling, prec, out,
           nat, onat, wnat, cs, ps, fld, wr, arrived, wgt, gf, ret, xs, xr, ys, yr,
           load, hsend, hrecv, wsend, wrecv, msend, mrecv):
    steps, groups, cx, cy = wr.shape[0] // 2, wr.shape[1], wr.shape[2], wr.shape[4]
    variables = fld.shape[1]
    span = GROUP * cx
    end = windows - 1
    moved, edge, back0 = steps, steps + 1, steps + 2
    helping = keep < groups
    k = lax.axis_index("win")
    t = lax.axis_index("tile")
    before_x, after_x = lax.rem(t + tiles - TY, tiles), lax.rem(t + TY, tiles)
    before_y, after_y = lax.rem(t + tiles - 1, tiles), lax.rem(t + 1, tiles)
    around = (before_x, after_x, before_y, after_y)
    lender = end - 2
    is_first, is_last, lends = k == 0, k == end, k == lender
    lo, hi = jnp.where(is_last, keep, 0), jnp.where(lends, keep, groups)
    sel = jnp.where(is_last, 1, 0)
    nxt = jnp.where(is_last, lender + 1, k + 1)
    lone = jnp.where(is_last, 0, jnp.where(lends, keep, groups))

    def when(cond):
        return pl.when(cond)

    def part(g):
        return pl.ds(pl.multiple_of(g * span, span), span)

    def state_in(g):
        return pltpu.make_async_copy(state.at[:, part(g)], nat.at[:, part(g)], load.at[g])

    def winds_in(n):
        return pltpu.make_async_copy(winds.at[pl.ds(2 * n, 2)], wnat.at[pl.ds(2 * n, 2)], load.at[groups + n])

    obs_in = pltpu.make_async_copy(obs, onat, load.at[groups + steps])
    prec_in = pltpu.make_async_copy(prec, ps, load.at[groups + steps + 1])
    coupling_in = pltpu.make_async_copy(coupling, cs, load.at[groups + steps + 2])

    order = tuple(range(keep, groups)) + tuple(range(keep))
    for g in order:
        state_in(g).start()
    coupling_in.start()

    @when(~is_last)
    def _():
        for n in range(steps):
            winds_in(n).start()
    prec_in.start()
    obs_in.start()

    barrier = pltpu.get_barrier_semaphore()

    def greet(win, others):
        pl.semaphore_signal(barrier, inc=1, device_id={"win": win})
        for other in others:
            pl.semaphore_signal(barrier, inc=1, device_id={"win": win, "tile": other})

    for other in around:
        pl.semaphore_signal(barrier, inc=1, device_id={"tile": other})

    @when(k < end)
    def _():
        greet(k + 1, around)

    @when(k > 0)
    def _():
        greet(k - 1, around)

    met = 4 + 5 * jnp.where(k < end, 1, 0) + 5 * jnp.where(k > 0, 1, 0)
    if helping:
        @when(lends)
        def _():
            greet(end, ())

        @when(is_last)
        def _():
            greet(lender, ())
        met = met + jnp.where(lends | is_last, 1, 0)

    shape = (GROUP, cy)
    lane = lax.broadcasted_iota(jnp.int32, shape, 1)
    level = lax.broadcasted_iota(jnp.int32, shape, 0)
    pair, odd = lane // 2, lane % 2 == 1
    at_start, at_end = lane == 0, lane == cy - 1

    def halo(slot, g, win, low, high):
        made = []
        for side, to in enumerate((before_y, after_y)):
            made.append(pltpu.make_async_remote_copy(
                src_ref=ys.at[slot, g], dst_ref=yr.at[slot, side, g],
                send_sem=hsend.at[slot, side, g], recv_sem=hrecv.at[slot, side, g],
                device_id={"win": win, "tile": to}))
        for side, (to, rows) in enumerate(((before_x, low), (after_x, high))):
            made.append(pltpu.make_async_remote_copy(
                src_ref=rows, dst_ref=xr.at[slot, side, g],
                send_sem=hsend.at[slot, 2 + side, g], recv_sem=hrecv.at[slot, 2 + side, g],
                device_id={"win": win, "tile": to}))
        return made

    def field_halo(slot, g, win, index):
        return halo(slot, g, win, fld.at[index, :, g, 0], fld.at[index, :, g, cx - 1])

    def flux_halo(slot, g):
        return halo(slot, g, k, xs.at[slot - back0, 0, g], xs.at[slot - back0, 1, g])

    def receive(slot, g):
        for copy in halo(slot, g, k, xr.at[slot, 0, g], xr.at[slot, 1, g]):
            copy.wait_recv()

    def onward(g):
        return pltpu.make_async_remote_copy(
            src_ref=fld.at[steps + 1, :, g], dst_ref=arrived.at[:, g],
            send_sem=wsend.at[0, g], recv_sem=wrecv.at[0, g], device_id={"win": nxt})

    def back(g):
        source = jnp.where((k == lender + 1) & (g >= keep), end, k - 1)
        return pltpu.make_async_remote_copy(
            src_ref=wgt.at[:, g], dst_ref=gf.at[0, :, g],
            send_sem=wsend.at[1, g], recv_sem=wrecv.at[1, g], device_id={"win": source})

    def lend_state(g):
        return pltpu.make_async_remote_copy(
            src_ref=fld.at[0, :, g], dst_ref=fld.at[1, :, g],
            send_sem=msend.at[0, g], recv_sem=mrecv.at[0, g], device_id={"win": end})

    def lend_winds(n, g):
        return pltpu.make_async_remote_copy(
            src_ref=wr.at[pl.ds(2 * n, 2), g], dst_ref=wr.at[pl.ds(2 * n, 2), g],
            send_sem=msend.at[2 + n, g], recv_sem=mrecv.at[2 + n, g], device_id={"win": end})

    def give_back(g):
        return pltpu.make_async_remote_copy(
            src_ref=ret.at[:, g], dst_ref=ret.at[:, g],
            send_sem=msend.at[1, g], recv_sem=mrecv.at[1, g], device_id={"win": lender})

    def place(v, r):
        return v * cx + r

    def pack(packed, value, v, r):
        p = place(v, r)
        return jnp.where(pair == p, pltpu.roll(value, 2 * p + 1, 1), packed)

    def rims(north, south):
        return jnp.where(odd, north, pltpu.roll(south, 2, 1))

    def sides(value, rim, v, r):
        edge_pair = pltpu.roll(rim, cy - 2 - 2 * place(v, r), 1)
        north = jnp.where(at_end, edge_pair, pltpu.roll(value, cy - 1, 1))
        south = jnp.where(at_start, edge_pair, pltpu.roll(value, 1, 1))
        return north, south

    def every(f):
        for v in range(variables):
            f(v)

    def rows_of(g, r):
        return pl.ds(g * span + r, GROUP, stride=cx)

    def convert_state(g):
        for v in range(variables):
            for r in range(cx):
                fld[0, v, g, r] = nat[v, rows_of(g, r), :]

    def pack_state(g, index, slot):
        packed = jnp.zeros(shape, jnp.float32)
        for v in range(variables):
            for r in range(cx):
                packed = pack(packed, fld[index, v, g, r], v, r)
        ys[slot, g] = packed

    def over(a, b, f):
        lax.fori_loop(a, b, lambda g, c: (f(g), c)[1], 0)

    for g in order:
        state_in(g).wait()
        convert_state(g)
        if g == order[0]:
            pl.semaphore_wait(barrier, met)
        if g >= keep:
            @when(lends)
            def _():
                lend_state(g).start()

        @when((k < end) & (g < hi))
        def _():
            pack_state(g, 0, 0)
            for copy in field_halo(0, g, k, 0):
                copy.start()

    def convert_winds(n, g):
        for way in range(2):
            for j in range(GROUP):
                tile = wnat[2 * n + way, g * GROUP + j].astype(jnp.float32)
                for r in range(cx):
                    wr[2 * n + way, g, r, pl.ds(j, 1), :] = tile[r:r + 1]

    @when(k < end)
    def _():
        for n in range(steps):
            winds_in(n).wait()

            def one(i, n=n):
                g = lax.rem(i + keep, groups)
                convert_winds(n, g)
                if helping:
                    @when(lends & (g >= keep))
                    def _():
                        lend_winds(n, g).start()
            over(0, groups, one)

    coupling_in.wait()

    if helping:
        @when(is_last)
        def _():
            @functools.partial(over, keep, groups)
            def _(g):
                lend_state(g).wait_recv()
                pack_state(g, 1, 0)
                for copy in field_halo(0, g, k, 1):
                    copy.start()

    def ship_edge(g):
        pack_state(g, 0, edge)
        for copy in field_halo(edge, g, k, 0):
            copy.start()

    def forward(n, g):
        if helping:
            @when(is_last)
            def _():
                lend_winds(n, g).wait_recv()
        receive(n, g)
        source = jnp.where(n == 0, sel, n + 1)
        rim = rims(yr[n, 0, g], yr[n, 1, g])

        def row(r):
            if r < 0:
                return [xr[n, 1, g, v] for v in range(variables)]
            if r == cx:
                return [xr[n, 0, g, v] for v in range(variables)]
            return [fld[source, v, g, r] for v in range(variables)]

        west, here = row(-1), row(0)
        packed = jnp.zeros(shape, jnp.float32)
        for r in range(cx):
            east = row(r + 1)
            u, w = wr[2 * n, g, r], wr[2 * n + 1, g, r]
            for v in range(variables):
                north, south = sides(here[v], rim, v, r)
                total = here[v] + u * (east[v] - west[v]) + w * (north - south)
                for b in range(variables):
                    total = total + cs[v, b] * here[b]
                fld[n + 2, v, g, r] = total
                packed = pack(packed, total, v, r)
            west, here = here, east
        ys[n + 1, g] = packed
        ends = n == steps - 1
        for copy in field_halo(n + 1, g, jnp.where(ends, nxt, k), n + 2):
            copy.start()

        @when(ends)
        def _():
            onward(g).start()

    @functools.partial(over, 0, steps)
    def _(n):
        @when(n == min(1, steps - 1))
        def _():
            over(lone, groups, ship_edge)
        over(lo, hi, lambda g: forward(n, g))

    prec_in.wait()

    def stencil(g, row, rim):
        scale = []
        for v in range(variables):
            s = jnp.zeros(shape, jnp.float32)
            for j in range(GROUP):
                s = jnp.where(level == j, ps[v, g * GROUP + j], s)
            scale.append(s)
        west, here = row(-1), row(0)
        for r in range(cx):
            east = row(r + 1)
            for v in range(variables):
                north, south = sides(here[v], rim, v, r)
                smooth = (1.0 + 4.0 * smooth_weight) * here[v] - smooth_weight * (
                    east[v] + west[v] + north + south)
                wgt[v, g, r] = scale[v] * smooth
            west, here = here, east

    def start_window(g):
        def row(r):
            if r < 0:
                return [xr[0, 1, g, v] for v in range(variables)]
            if r == cx:
                return [xr[0, 0, g, v] for v in range(variables)]
            return [fld[0, v, g, r] for v in range(variables)]
        stencil(g, row, rims(yr[0, 0, g], yr[0, 1, g]))

    def mismatch(g):
        edges = jnp.where(g >= lone, edge, 0)

        @when(g >= lone)
        def _():
            receive(edge, g)
        receive(moved, g)
        onward(g).wait_recv()

        def row(r):
            if r < 0:
                return [xr[edges, 1, g, v] - xr[moved, 1, g, v] for v in range(variables)]
            if r == cx:
                return [xr[edges, 0, g, v] - xr[moved, 0, g, v] for v in range(variables)]
            return [fld[0, v, g, r] - arrived[v, g, r] for v in range(variables)]
        stencil(g, row, rims(yr[edges, 0, g] - yr[moved, 0, g], yr[edges, 1, g] - yr[moved, 1, g]))
        back(g).start()

    @when(k > 0)
    def _():
        over(0, groups, mismatch)

    @when(is_first)
    def _():
        over(0, groups, start_window)

    def begin_back(g):
        back(g).wait_recv()
        n = steps - 1
        packed = jnp.zeros(shape, jnp.float32)
        for r in range(cx):
            u, w = wr[2 * n, g, r], wr[2 * n + 1, g, r]
            for v in range(variables):
                value = gf[0, v, g, r]
                if r == 0:
                    xs[0, 0, g, v] = u * value
                if r == cx - 1:
                    xs[0, 1, g, v] = u * value
                packed = pack(packed, w * value, v, r)
        ys[back0, g] = packed
        for copy in flux_halo(back0, g):
            copy.start()

    def backward(i, g, final):
        n = steps - 1 - i
        slot = back0 + i
        receive(slot, g)
        rim = rims(yr[slot, 0, g], yr[slot, 1, g])

        def row(r):
            if r < 0:
                return None, [xr[slot, 1, g, v] for v in range(variables)]
            if r == cx:
                return None, [xr[slot, 0, g, v] for v in range(variables)]
            u = wr[2 * n, g, r]
            values = [gf[i, v, g, r] for v in range(variables)]
            return values, [u * value for value in values]

        (_, west), (values, here) = row(-1), row(0)
        packed = jnp.zeros(shape, jnp.float32)
        for r in range(cx):
            values_east, east = row(r + 1)
            w = wr[2 * n + 1, g, r]
            if not final:
                u_next, w_next = wr[2 * n - 2, g, r], wr[2 * n - 1, g, r]
            for v in range(variables):
                north, south = sides(w * values[v], rim, v, r)
                total = values[v] + (west[v] - east[v]) + (south - north)
                for b in range(variables):
                    total = total + cs[b, v] * values[b]
                if final:
                    ret[v, g, r] = total
                    continue
                gf[i + 1, v, g, r] = total
                if r == 0:
                    xs[i + 1, 0, g, v] = u_next * total
                if r == cx - 1:
                    xs[i + 1, 1, g, v] = u_next * total
                packed = pack(packed, w_next * total, v, r)
            west, values, here = here, values_east, east
        if not final:
            ys[slot + 1, g] = packed
            for copy in flux_halo(slot + 1, g):
                copy.start()

    over(lo, hi, begin_back)

    @functools.partial(over, 0, steps - 1)
    def _(i):
        over(lo, hi, lambda g: backward(i, g, False))

    obs_in.wait()

    def finish(g, has_next):
        for v in range(variables):
            for r in range(cx):
                rows = rows_of(g, r)
                own = wgt[v, g, r] + onat[v, rows, :] * fld[0, v, g, r]
                out[v, rows, :] = own - ret[v, g, r] if has_next else own

    @functools.partial(over, lo, hi)
    def _(g):
        backward(steps - 1, g, True)

        @when(~is_last)
        def _():
            finish(g, True)
        if helping:
            @when(is_last)
            def _():
                give_back(g).start()

    @when(is_last)
    def _():
        @functools.partial(over, 0, groups)
        def _(g):
            finish(g, False)

    if helping:
        @when(lends)
        def _():
            @functools.partial(over, keep, groups)
            def _(g):
                give_back(g).wait_recv()
                finish(g, True)

    def sent(copies):
        for copy in copies:
            copy.wait_send()

    @functools.partial(over, lo, hi)
    def _(g):
        for n in range(steps + 1):
            sent(field_halo(n, g, k, 0))
        for i in range(steps):
            sent(flux_halo(back0 + i, g))
        onward(g).wait_send()

    @when(k > 0)
    def _():
        over(0, groups, lambda g: back(g).wait_send())

    over(lone, groups, lambda g: sent(field_halo(edge, g, k, 0)))
    if helping:
        @when(is_last)
        def _():
            over(keep, groups, lambda g: give_back(g).wait_send())

    if helping:
        @when(lends)
        def _():
            @functools.partial(over, keep, groups)
            def _(g):
                lend_state(g).wait_send()
                for n in range(steps):
                    lend_winds(n, g).wait_send()


def solution(mesh):
    windows, tiles = mesh.shape["win"], mesh.shape["tile"]

    def body(state, obs, trajectory, coupling, prec):
        block = state.shape[2:]
        variables, levels, cx, cy = block
        steps = trajectory.shape[2]
        groups = levels // GROUP
        keep = groups // 2 if windows > 3 else groups
        slots = 2 * steps + 2
        flat = (variables, levels * cx, cy)
        field = (variables, groups, cx, GROUP, cy)
        anywhere = pl.BlockSpec(memory_space=pltpu.HBM)
        f32 = jnp.float32
        result = pl.pallas_call(
            functools.partial(kernel, windows, tiles, keep),
            out_shape=jax.ShapeDtypeStruct(flat, f32),
            in_specs=[anywhere] * 5,
            out_specs=pl.BlockSpec(memory_space=pltpu.VMEM),
            scratch_shapes=[
                pltpu.VMEM(flat, f32),
                pltpu.VMEM(flat, f32),
                pltpu.VMEM((2 * steps, levels, cx, cy), trajectory.dtype),
                pltpu.SMEM(coupling.shape, f32),
                pltpu.SMEM(prec.shape, f32),
                pltpu.VMEM((steps + 2,) + field, f32),
                pltpu.VMEM((2 * steps, groups, cx, GROUP, cy), f32),
                pltpu.VMEM(field, f32),
                pltpu.VMEM(field, f32),
                pltpu.VMEM((steps,) + field, f32),
                pltpu.VMEM(field, f32),
                pltpu.VMEM((steps, 2, groups, variables, GROUP, cy), f32),
                pltpu.VMEM((slots, 2, groups, variables, GROUP, cy), f32),
                pltpu.VMEM((slots, groups, GROUP, cy), f32),
                pltpu.VMEM((slots, 2, groups, GROUP, cy), f32),
                pltpu.SemaphoreType.DMA((groups + steps + 3,)),
                pltpu.SemaphoreType.DMA((slots, 4, groups)),
                pltpu.SemaphoreType.DMA((slots, 4, groups)),
                pltpu.SemaphoreType.DMA((2, groups)),
                pltpu.SemaphoreType.DMA((2, groups)),
                pltpu.SemaphoreType.DMA((2 + steps, groups)),
                pltpu.SemaphoreType.DMA((2 + steps, groups)),
            ],
            compiler_params=pltpu.CompilerParams(
                collective_id=0, has_side_effects=True, vmem_limit_bytes=48 * 2**20),
        )(*[pltpu.with_memory_space_constraint(x, pltpu.HBM) for x in (
            state.reshape(flat), obs.reshape(flat),
            trajectory.reshape((2 * steps, levels, cx, cy)), coupling, prec)])
        return result.reshape((1, 1) + block)

    spec = P("win", "tile", None, None, None, None)
    return jax.shard_map(
        body, mesh=mesh,
        in_specs=(spec, spec, P("win", "tile", None, None, None, None, None), P(), P()),
        out_specs=spec, check_vma=False)
```

```python
import functools

import jax
import jax.numpy as jnp
from jax import lax
from jax.experimental import pallas as pl
from jax.experimental.pallas import tpu as pltpu
from jax.sharding import PartitionSpec as P

TY = 4
GROUP = 8

smooth_weight = 0.2


def kernel(windows, tiles, keep, hold, state, obs, winds, coupling, prec, out,
           nat, onat, wnat, cs, ps, fld, wr, arrived, wgt, gf, ret, xs, xr, ys, yr, xw, xe, ye,
           load, hsend, hrecv, wsend, wrecv, msend, mrecv, esend, erecv):
    steps, groups, cx, cy = wr.shape[0] // 2, wr.shape[1], wr.shape[2], wr.shape[4]
    variables = fld.shape[1]
    span = GROUP * cx
    end = windows - 1
    gap, back0 = steps, steps + 1
    breeze, early = back0 + steps, back0 + steps + 1
    helping = keep < groups
    k = lax.axis_index("win")
    t = lax.axis_index("tile")
    before_x, after_x = lax.rem(t + tiles - TY, tiles), lax.rem(t + TY, tiles)
    before_y, after_y = lax.rem(t + tiles - 1, tiles), lax.rem(t + 1, tiles)
    around = (before_x, after_x, before_y, after_y)
    lender = end - 2
    is_first, is_last, lends = k == 0, k == end, k == lender
    lo, hi = jnp.where(is_last, keep, 0), jnp.where(lends, keep, groups)
    back_lo, back_hi = jnp.where(is_last, hold, 0), jnp.where(lends, hold, groups)
    sel = jnp.where(is_last, 1, 0)
    nxt = jnp.where(is_last, lender + 1, k + 1)

    def when(cond):
        return pl.when(cond)

    def part(g):
        return pl.ds(pl.multiple_of(g * span, span), span)

    def state_in(g):
        return pltpu.make_async_copy(state.at[:, part(g)], nat.at[:, part(g)], load.at[g])

    def winds_in(n):
        return pltpu.make_async_copy(winds.at[pl.ds(2 * n, 2)], wnat.at[pl.ds(2 * n, 2)], load.at[groups + n])

    obs_in = pltpu.make_async_copy(obs, onat, load.at[groups + steps])
    prec_in = pltpu.make_async_copy(prec, ps, load.at[groups + steps + 1])
    coupling_in = pltpu.make_async_copy(coupling, cs, load.at[groups + steps + 2])

    order = tuple(range(keep, groups)) + tuple(range(keep))
    for g in order:
        state_in(g).start()
    coupling_in.start()

    @when(~is_last)
    def _():
        for n in range(steps):
            winds_in(n).start()
    prec_in.start()
    obs_in.start()

    barrier = pltpu.get_barrier_semaphore()

    def greet(win, others):
        pl.semaphore_signal(barrier, inc=1, device_id={"win": win})
        for other in others:
            pl.semaphore_signal(barrier, inc=1, device_id={"win": win, "tile": other})

    for other in around:
        pl.semaphore_signal(barrier, inc=1, device_id={"tile": other})

    @when(k < end)
    def _():
        greet(k + 1, around)

    @when(k > 0)
    def _():
        greet(k - 1, around)

    met = 4 + 5 * jnp.where(k < end, 1, 0) + 5 * jnp.where(k > 0, 1, 0)
    if helping:
        @when(lends)
        def _():
            greet(end, ())

        @when(is_last)
        def _():
            greet(lender, ())
        met = met + jnp.where(lends | is_last, 1, 0)

    shape = (GROUP, cy)
    lane = lax.broadcasted_iota(jnp.int32, shape, 1)
    level = lax.broadcasted_iota(jnp.int32, shape, 0)
    pair, odd = lane // 2, lane % 2 == 1
    at_start, at_end = lane == 0, lane == cy - 1

    def halo(slot, g, win, low, high, into=None):
        into = xr.at[slot] if into is None else into
        made = []
        for side, to in enumerate((before_y, after_y)):
            made.append(pltpu.make_async_remote_copy(
                src_ref=ys.at[slot, g], dst_ref=yr.at[slot, side, g],
                send_sem=hsend.at[slot, side, g], recv_sem=hrecv.at[slot, side, g],
                device_id={"win": win, "tile": to}))
        for side, (to, rows) in enumerate(((before_x, low), (after_x, high))):
            made.append(pltpu.make_async_remote_copy(
                src_ref=rows, dst_ref=into.at[side, g],
                send_sem=hsend.at[slot, 2 + side, g], recv_sem=hrecv.at[slot, 2 + side, g],
                device_id={"win": win, "tile": to}))
        return made

    def field_halo(slot, g, index):
        return halo(slot, g, k, fld.at[index, :, g, 0], fld.at[index, :, g, cx - 1])

    def gap_halo(g):
        return halo(gap, g, nxt, xs.at[0, 0, g], xs.at[0, 1, g])

    def weighted_halo(g):
        return halo(back0, g, source(g, hold), wgt.at[:, g, 0], wgt.at[:, g, cx - 1])

    def flux_halo(i, g):
        return halo(back0 + i, g, k, xs.at[i, 0, g], xs.at[i, 1, g])

    def breeze_halo(g):
        u = wr.at[2 * steps - 2, g]
        return halo(breeze, g, k, u.at[0], u.at[cx - 1], xw)

    def receive(slot, g):
        for copy in halo(slot, g, k, xr.at[slot, 0, g], xr.at[slot, 1, g]):
            copy.wait_recv()

    def source(g, bound):
        return jnp.where((k == lender + 1) & (g >= bound), end, k - 1)

    def early_edges(g):
        made = []
        for i, (src, dst) in enumerate((
            (fld.at[0, :, g, 0], xe.at[0, g]), (fld.at[0, :, g, cx - 1], xe.at[1, g]), (ys.at[early, g], ye.at[g]),
        )):
            made.append(pltpu.make_async_remote_copy(
                src_ref=src, dst_ref=dst, send_sem=esend.at[i, g], recv_sem=erecv.at[i, g],
                device_id={"win": source(g, keep)}))
        return made

    def onward(g):
        return pltpu.make_async_remote_copy(
            src_ref=fld.at[steps + 1, :, g], dst_ref=arrived.at[:, g],
            send_sem=wsend.at[0, g], recv_sem=wrecv.at[0, g], device_id={"win": nxt})

    def back(g):
        return pltpu.make_async_remote_copy(
            src_ref=wgt.at[:, g], dst_ref=gf.at[0, :, g],
            send_sem=wsend.at[1, g], recv_sem=wrecv.at[1, g], device_id={"win": source(g, hold)})

    def lend_state(g):
        return pltpu.make_async_remote_copy(
            src_ref=fld.at[0, :, g], dst_ref=fld.at[1, :, g],
            send_sem=msend.at[0, g], recv_sem=mrecv.at[0, g], device_id={"win": end})

    def lend_winds(n, g):
        return pltpu.make_async_remote_copy(
            src_ref=wr.at[pl.ds(2 * n, 2), g], dst_ref=wr.at[pl.ds(2 * n, 2), g],
            send_sem=msend.at[2 + n, g], recv_sem=mrecv.at[2 + n, g], device_id={"win": end})

    def give_back(g):
        return pltpu.make_async_remote_copy(
            src_ref=ret.at[:, g], dst_ref=ret.at[:, g],
            send_sem=msend.at[1, g], recv_sem=mrecv.at[1, g], device_id={"win": lender})

    def place(v, r):
        return v * cx + r

    def pack(packed, value, v, r):
        p = place(v, r)
        return jnp.where(pair == p, pltpu.roll(value, 2 * p + 1, 1), packed)

    def rims(north, south):
        return jnp.where(odd, north, pltpu.roll(south, 2, 1))

    def sides(value, rim, v, r):
        edge_pair = pltpu.roll(rim, cy - 2 - 2 * place(v, r), 1)
        north = jnp.where(at_end, edge_pair, pltpu.roll(value, cy - 1, 1))
        south = jnp.where(at_start, edge_pair, pltpu.roll(value, 1, 1))
        return north, south

    def every(f):
        for v in range(variables):
            f(v)

    def rows_of(g, r):
        return pl.ds(g * span + r, GROUP, stride=cx)

    def convert_state(g):
        for v in range(variables):
            for r in range(cx):
                fld[0, v, g, r] = nat[v, rows_of(g, r), :]

    def pack_state(g, index):
        packed = jnp.zeros(shape, jnp.float32)
        for v in range(variables):
            for r in range(cx):
                packed = pack(packed, fld[index, v, g, r], v, r)
        return packed

    def start(copies):
        for copy in copies:
            copy.start()

    def over(a, b, f):
        lax.fori_loop(a, b, lambda g, c: (f(g), c)[1], 0)

    for g in order:
        state_in(g).wait()
        convert_state(g)
        if g == order[0]:
            pl.semaphore_wait(barrier, met)
        if g >= keep:
            @when(lends)
            def _():
                lend_state(g).start()

        packed = pack_state(g, 0)
        ys[0, g] = packed
        ys[early, g] = packed

        @when((k < end) & (g < hi))
        def _():
            start(field_halo(0, g, 0))

    @when(k > 0)
    def _():
        over(0, groups, lambda g: start(early_edges(g)))

    def convert_winds(n, g):
        for way in range(2):
            for j in range(GROUP):
                tile = wnat[2 * n + way, g * GROUP + j].astype(jnp.float32)
                for r in range(cx):
                    wr[2 * n + way, g, r, pl.ds(j, 1), :] = tile[r:r + 1]

    @when(k < end)
    def _():
        for n in range(steps):
            winds_in(n).wait()

            def one(i, n=n):
                g = lax.rem(i + keep, groups)
                convert_winds(n, g)
                if helping:
                    @when(lends & (g >= keep))
                    def _():
                        lend_winds(n, g).start()
            over(0, groups, one)

    coupling_in.wait()

    if helping:
        @when(is_last)
        def _():
            @functools.partial(over, keep, groups)
            def _(g):
                lend_state(g).wait_recv()
                ys[0, g] = pack_state(g, 1)
                start(field_halo(0, g, 1))

    def ship_breeze(g):
        n = steps - 1
        packed = jnp.zeros(shape, jnp.float32)
        for r in range(cx):
            packed = pack(packed, wr[2 * n + 1, g, r], 0, r)
        total = packed
        for v in range(1, variables):
            total = total + pltpu.roll(packed, 2 * place(v, 0), 1)
        ys[breeze, g] = total
        start(breeze_halo(g))

    def forward(n, g, final):
        if not final:
            if helping:
                @when(is_last)
                def _():
                    lend_winds(n, g).wait_recv()
        receive(n, g)
        index = jnp.where(n == 0, sel, n + 1)
        rim = rims(yr[n, 0, g], yr[n, 1, g])
        if final:
            for copy in early_edges(g):
                copy.wait_recv()

        def row(r):
            if r < 0:
                return [xr[n, 1, g, v] for v in range(variables)]
            if r == cx:
                return [xr[n, 0, g, v] for v in range(variables)]
            return [fld[index, v, g, r] for v in range(variables)]

        west, here = row(-1), row(0)
        packed = jnp.zeros(shape, jnp.float32)
        for r in range(cx):
            east = row(r + 1)
            u, w = wr[2 * n, g, r], wr[2 * n + 1, g, r]
            for v in range(variables):
                north, south = sides(here[v], rim, v, r)
                total = here[v] + u * (east[v] - west[v]) + w * (north - south)
                for b in range(variables):
                    total = total + cs[v, b] * here[b]
                fld[n + 2, v, g, r] = total
                if final and r == 0:
                    xs[0, 0, g, v] = xe[0, g, v] - total
                if final and r == cx - 1:
                    xs[0, 1, g, v] = xe[1, g, v] - total
                packed = pack(packed, total, v, r)
            west, here = here, east
        if final:
            ys[gap, g] = ye[g] - packed
            start(gap_halo(g))
            onward(g).start()
        else:
            ys[n + 1, g] = packed
            start(field_halo(n + 1, g, n + 2))

    def ship_breezes():
        if helping:
            @when(is_last)
            def _():
                over(keep, groups, lambda g: lend_winds(steps - 1, g).wait_recv())
        over(back_lo, back_hi, ship_breeze)

    @functools.partial(over, 0, steps - 1)
    def _(n):
        @when(n == min(1, steps - 2))
        def _():
            ship_breezes()
        over(lo, hi, lambda g: forward(n, g, False))

    if steps < 2:
        ship_breezes()
    over(lo, hi, lambda g: forward(steps - 1, g, True))

    prec_in.wait()

    def stencil(g, row, rim, keeps):
        scale = []
        for v in range(variables):
            s = jnp.zeros(shape, jnp.float32)
            for j in range(GROUP):
                s = jnp.where(level == j, ps[v, g * GROUP + j], s)
            scale.append(s)
        west, here = row(-1), row(0)
        packed = jnp.zeros(shape, jnp.float32)
        for r in range(cx):
            east = row(r + 1)
            for v in range(variables):
                north, south = sides(here[v], rim, v, r)
                smooth = (1.0 + 4.0 * smooth_weight) * here[v] - smooth_weight * (
                    east[v] + west[v] + north + south)
                total = scale[v] * smooth
                wgt[v, g, r] = total
                if keeps:
                    packed = pack(packed, total, v, r)
            west, here = here, east
        return packed

    def start_window(g):
        def row(r):
            if r < 0:
                return [xr[0, 1, g, v] for v in range(variables)]
            if r == cx:
                return [xr[0, 0, g, v] for v in range(variables)]
            return [fld[0, v, g, r] for v in range(variables)]
        stencil(g, row, rims(yr[0, 0, g], yr[0, 1, g]), False)

    def mismatch(g):
        receive(gap, g)
        onward(g).wait_recv()

        def row(r):
            if r < 0:
                return [xr[gap, 1, g, v] for v in range(variables)]
            if r == cx:
                return [xr[gap, 0, g, v] for v in range(variables)]
            return [fld[0, v, g, r] - arrived[v, g, r] for v in range(variables)]
        ys[back0, g] = stencil(g, row, rims(yr[gap, 0, g], yr[gap, 1, g]), True)
        start(weighted_halo(g))
        back(g).start()

    @when(k > 0)
    def _():
        over(0, groups, mismatch)

    @when(is_first)
    def _():
        over(0, groups, start_window)

    def backward(i, g):
        n = steps - 1 - i
        slot = back0 + i
        first, final = i == 0, i == steps - 1
        if first:
            for copy in breeze_halo(g):
                copy.wait_recv()
            back(g).wait_recv()
        receive(slot, g)
        rim = [yr[slot, side, g] for side in range(2)]
        if first:
            rim = [rim[side] * yr[breeze, side, g] for side in range(2)]
        rim = rims(*rim)

        def beyond(side):
            values = [xr[slot, side, g, v] for v in range(variables)]
            return [value * xw[side, g] for value in values] if first else values

        def row(r):
            if r < 0:
                return None, beyond(1)
            if r == cx:
                return None, beyond(0)
            u = wr[2 * n, g, r]
            values = [gf[i, v, g, r] for v in range(variables)]
            return values, [u * value for value in values]

        (_, west), (values, here) = row(-1), row(0)
        packed = jnp.zeros(shape, jnp.float32)
        for r in range(cx):
            values_east, east = row(r + 1)
            w = wr[2 * n + 1, g, r]
            if not final:
                u_next, w_next = wr[2 * n - 2, g, r], wr[2 * n - 1, g, r]
            for v in range(variables):
                north, south = sides(w * values[v], rim, v, r)
                total = values[v] + (west[v] - east[v]) + (south - north)
                for b in range(variables):
                    total = total + cs[b, v] * values[b]
                if final:
                    ret[v, g, r] = total
                    continue
                gf[i + 1, v, g, r] = total
                if r == 0:
                    xs[i + 1, 0, g, v] = u_next * total
                if r == cx - 1:
                    xs[i + 1, 1, g, v] = u_next * total
                packed = pack(packed, w_next * total, v, r)
            west, values, here = here, values_east, east
        if not final:
            ys[slot + 1, g] = packed
            start(flux_halo(i + 1, g))

    for i in range(steps - 1):
        over(back_lo, back_hi, functools.partial(backward, i))

    obs_in.wait()

    def finish(g, has_next):
        for v in range(variables):
            for r in range(cx):
                rows = rows_of(g, r)
                own = wgt[v, g, r] + onat[v, rows, :] * fld[0, v, g, r]
                out[v, rows, :] = own - ret[v, g, r] if has_next else own

    @functools.partial(over, back_lo, back_hi)
    def _(g):
        backward(steps - 1, g)

        @when(~is_last)
        def _():
            finish(g, True)
        if helping:
            @when(is_last)
            def _():
                give_back(g).start()

    @when(is_last)
    def _():
        @functools.partial(over, 0, groups)
        def _(g):
            finish(g, False)

    if helping:
        @when(lends)
        def _():
            @functools.partial(over, hold, groups)
            def _(g):
                give_back(g).wait_recv()
                finish(g, True)

    def sent(copies):
        for copy in copies:
            copy.wait_send()

    @functools.partial(over, lo, hi)
    def _(g):
        for n in range(steps):
            sent(field_halo(n, g, 0))
        sent(gap_halo(g))
        onward(g).wait_send()

    @functools.partial(over, back_lo, back_hi)
    def _(g):
        for i in range(1, steps):
            sent(flux_halo(i, g))
        sent(breeze_halo(g))

    @when(k > 0)
    def _():
        @functools.partial(over, 0, groups)
        def _(g):
            sent(weighted_halo(g))
            sent(early_edges(g))
            back(g).wait_send()

    if helping:
        @when(is_last)
        def _():
            over(hold, groups, lambda g: give_back(g).wait_send())

    if helping:
        @when(lends)
        def _():
            @functools.partial(over, keep, groups)
            def _(g):
                lend_state(g).wait_send()
                for n in range(steps):
                    lend_winds(n, g).wait_send()


def solution(mesh):
    windows, tiles = mesh.shape["win"], mesh.shape["tile"]

    def body(state, obs, trajectory, coupling, prec):
        block = state.shape[2:]
        variables, levels, cx, cy = block
        steps = trajectory.shape[2]
        groups = levels // GROUP
        keep, hold = (groups // 2, groups - groups // 4) if windows > 3 else (groups, groups)
        slots = 2 * steps + 3
        flat = (variables, levels * cx, cy)
        field = (variables, groups, cx, GROUP, cy)
        anywhere = pl.BlockSpec(memory_space=pltpu.HBM)
        f32 = jnp.float32
        result = pl.pallas_call(
            functools.partial(kernel, windows, tiles, keep, hold),
            out_shape=jax.ShapeDtypeStruct(flat, f32),
            in_specs=[anywhere] * 5,
            out_specs=pl.BlockSpec(memory_space=pltpu.VMEM),
            scratch_shapes=[
                pltpu.VMEM(flat, f32),
                pltpu.VMEM(flat, f32),
                pltpu.VMEM((2 * steps, levels, cx, cy), trajectory.dtype),
                pltpu.SMEM(coupling.shape, f32),
                pltpu.SMEM(prec.shape, f32),
                pltpu.VMEM((steps + 2,) + field, f32),
                pltpu.VMEM((2 * steps, groups, cx, GROUP, cy), f32),
                pltpu.VMEM(field, f32),
                pltpu.VMEM(field, f32),
                pltpu.VMEM((steps,) + field, f32),
                pltpu.VMEM(field, f32),
                pltpu.VMEM((steps, 2, groups, variables, GROUP, cy), f32),
                pltpu.VMEM((slots, 2, groups, variables, GROUP, cy), f32),
                pltpu.VMEM((slots, groups, GROUP, cy), f32),
                pltpu.VMEM((slots, 2, groups, GROUP, cy), f32),
                pltpu.VMEM((2, groups, GROUP, cy), f32),
                pltpu.VMEM((2, groups, variables, GROUP, cy), f32),
                pltpu.VMEM((groups, GROUP, cy), f32),
                pltpu.SemaphoreType.DMA((groups + steps + 3,)),
                pltpu.SemaphoreType.DMA((slots, 4, groups)),
                pltpu.SemaphoreType.DMA((slots, 4, groups)),
                pltpu.SemaphoreType.DMA((2, groups)),
                pltpu.SemaphoreType.DMA((2, groups)),
                pltpu.SemaphoreType.DMA((2 + steps, groups)),
                pltpu.SemaphoreType.DMA((2 + steps, groups)),
                pltpu.SemaphoreType.DMA((3, groups)),
                pltpu.SemaphoreType.DMA((3, groups)),
            ],
            compiler_params=pltpu.CompilerParams(
                collective_id=0, has_side_effects=True, vmem_limit_bytes=48 * 2**20),
        )(*[pltpu.with_memory_space_constraint(x, pltpu.HBM) for x in (
            state.reshape(flat), obs.reshape(flat),
            trajectory.reshape((2 * steps, levels, cx, cy)), coupling, prec)])
        return result.reshape((1, 1) + block)

    spec = P("win", "tile", None, None, None, None)
    return jax.shard_map(
        body, mesh=mesh,
        in_specs=(spec, spec, P("win", "tile", None, None, None, None, None), P(), P()),
        out_specs=spec, check_vma=False)
```

```python
import functools

import jax
import jax.numpy as jnp
from jax import lax
from jax.experimental import pallas as pl
from jax.experimental.pallas import tpu as pltpu
from jax.sharding import PartitionSpec as P

TY = 4
GROUP = 8

smooth_weight = 0.2


def kernel(windows, tiles, keep, hold, state, obs, winds, coupling, prec, out,
           nat, onat, wnat, cs, ps, fld, wr, arrived, wgt, gf, ret, xs, xr, ys, yr, yp, xe, ye, xw, yw,
           load, hsend, hrecv, wsend, wrecv, msend, mrecv, esend, erecv, fsend, frecv):
    steps, groups, cx, cy = wr.shape[0] // 2, wr.shape[1], wr.shape[2], wr.shape[4]
    variables = fld.shape[1]
    span = GROUP * cx
    end = windows - 1
    gap, back0 = steps, steps + 1
    half = GROUP // 2
    helping = keep < groups
    k = lax.axis_index("win")
    t = lax.axis_index("tile")
    before_x, after_x = lax.rem(t + tiles - TY, tiles), lax.rem(t + TY, tiles)
    before_y, after_y = lax.rem(t + tiles - 1, tiles), lax.rem(t + 1, tiles)
    around = (before_x, after_x, before_y, after_y)
    lender = end - 2
    is_first, is_last, lends = k == 0, k == end, k == lender
    lo, hi = jnp.where(is_last, keep, 0), jnp.where(lends, keep, groups)
    back_lo, back_hi = jnp.where(is_last, hold, 0), jnp.where(lends, hold, groups)
    sel = jnp.where(is_last, 1, 0)
    nxt = jnp.where(is_last, lender + 1, k + 1)

    def when(cond):
        return pl.when(cond)

    def part(g):
        return pl.ds(pl.multiple_of(g * span, span), span)

    def state_in(g):
        return pltpu.make_async_copy(state.at[:, part(g)], nat.at[:, part(g)], load.at[g])

    def winds_in(n):
        return pltpu.make_async_copy(winds.at[pl.ds(2 * n, 2)], wnat.at[pl.ds(2 * n, 2)], load.at[groups + n])

    obs_in = pltpu.make_async_copy(obs, onat, load.at[groups + steps])
    prec_in = pltpu.make_async_copy(prec, ps, load.at[groups + steps + 1])
    coupling_in = pltpu.make_async_copy(coupling, cs, load.at[groups + steps + 2])

    order = tuple(range(keep, groups)) + tuple(range(keep))
    for g in order:
        state_in(g).start()
    coupling_in.start()

    @when(~is_last)
    def _():
        for n in range(steps):
            winds_in(n).start()
    prec_in.start()
    obs_in.start()

    barrier = pltpu.get_barrier_semaphore()

    def greet(win):
        pl.semaphore_signal(barrier, inc=1, device_id={"win": win})

    for other in around:
        pl.semaphore_signal(barrier, inc=1, device_id={"tile": other})

    @when(k < end)
    def _():
        greet(k + 1)

    @when(k > 0)
    def _():
        greet(k - 1)

    met = len(around) + jnp.where(k < end, 1, 0) + jnp.where(k > 0, 1, 0)
    if helping:
        @when(lends)
        def _():
            greet(end)

        @when(is_last)
        def _():
            greet(lender)
        met = met + jnp.where(lends | is_last, 1, 0)

    shape = (GROUP, cy)
    lane = lax.broadcasted_iota(jnp.int32, shape, 1)
    level = lax.broadcasted_iota(jnp.int32, shape, 0)
    pair, odd = lane // 2, lane % 2 == 1
    at_start, at_end = lane == 0, lane == cy - 1

    def halo(slot, g, win, low, high):
        made = []
        for side, to in enumerate((before_y, after_y)):
            made.append(pltpu.make_async_remote_copy(
                src_ref=ys.at[slot, side, g], dst_ref=yr.at[slot, side, g],
                send_sem=hsend.at[slot, side, g], recv_sem=hrecv.at[slot, side, g],
                device_id={"win": win, "tile": to}))
        for side, (to, rows) in enumerate(((before_x, low), (after_x, high))):
            made.append(pltpu.make_async_remote_copy(
                src_ref=rows, dst_ref=xr.at[slot, side, g],
                send_sem=hsend.at[slot, 2 + side, g], recv_sem=hrecv.at[slot, 2 + side, g],
                device_id={"win": win, "tile": to}))
        return made

    def field_halo(slot, g, index):
        return halo(slot, g, k, fld.at[index, :, g, 0], fld.at[index, :, g, cx - 1])

    def gap_halo(g):
        return halo(gap, g, nxt, xs.at[0, 0, g], xs.at[0, 1, g])

    def weighted_halo(g):
        return halo(back0, g, source(g, hold), xs.at[steps, 0, g], xs.at[steps, 1, g])

    def flux_halo(i, g):
        return halo(back0 + i, g, k, xs.at[i, 0, g], xs.at[i, 1, g])

    def receive(slot, g):
        for copy in halo(slot, g, k, xr.at[slot, 0, g], xr.at[slot, 1, g]):
            copy.wait_recv()

    def source(g, bound):
        return jnp.where((k == lender + 1) & (g >= bound), end, k - 1)

    def local_edges(pieces, sends, arrives, g, win):
        return [pltpu.make_async_remote_copy(
            src_ref=src, dst_ref=dst, send_sem=sends.at[i, g], recv_sem=arrives.at[i, g], device_id={"win": win})
            for i, (src, dst) in enumerate(pieces)]

    def state_edges(g):
        return local_edges((
            (fld.at[0, :, g, 0], xe.at[0, g]), (fld.at[0, :, g, cx - 1], xe.at[1, g]), (yp.at[0, g], ye.at[g]),
        ), esend, erecv, g, source(g, keep))

    def wind_edges(g):
        n = 2 * steps - 2
        return local_edges((
            (wr.at[n, g, 0], xw.at[0, g]), (wr.at[n, g, cx - 1], xw.at[1, g]), (yp.at[1, g], yw.at[g]),
        ), fsend, frecv, g, k + 1)

    def onward(g):
        return pltpu.make_async_remote_copy(
            src_ref=fld.at[steps + 1, :, g], dst_ref=arrived.at[:, g],
            send_sem=wsend.at[0, g], recv_sem=wrecv.at[0, g], device_id={"win": nxt})

    def back(g):
        return pltpu.make_async_remote_copy(
            src_ref=wgt.at[:, g], dst_ref=gf.at[0, :, g],
            send_sem=wsend.at[1, g], recv_sem=wrecv.at[1, g], device_id={"win": source(g, hold)})

    def lend_state(g):
        return pltpu.make_async_remote_copy(
            src_ref=fld.at[0, :, g], dst_ref=fld.at[1, :, g],
            send_sem=msend.at[0, g], recv_sem=mrecv.at[0, g], device_id={"win": end})

    def lend_winds(n, g):
        return pltpu.make_async_remote_copy(
            src_ref=wr.at[pl.ds(2 * n, 2), g], dst_ref=wr.at[pl.ds(2 * n, 2), g],
            send_sem=msend.at[2 + n, g], recv_sem=mrecv.at[2 + n, g], device_id={"win": end})

    def give_back(g):
        return pltpu.make_async_remote_copy(
            src_ref=ret.at[:, g], dst_ref=ret.at[:, g],
            send_sem=msend.at[1, g], recv_sem=mrecv.at[1, g], device_id={"win": lender})

    def place(v, r):
        return v * cx + r

    def pack(packed, value, v, r):
        p = place(v, r)
        return jnp.where(pair == p, pltpu.roll(value, 2 * p + 1, 1), packed)

    def fold(slot, g, packed):
        upper = pltpu.roll(pltpu.roll(packed, half, 0), 1, 1)
        ys[slot, 0, g] = jnp.where(odd, packed, upper)[:half]
        ys[slot, 1, g] = jnp.where(odd, upper, packed)[:half]

    def unfold(slot, g):
        north, south = [jnp.concatenate([yr[slot, side, g]] * 2, axis=0) for side in range(2)]
        north = jnp.where(level < half, north, pltpu.roll(north, cy - 1, 1))
        south = jnp.where(level < half, pltpu.roll(south, 2, 1), pltpu.roll(south, 1, 1))
        return jnp.where(odd, north, south)

    def sides(value, rim, v, r):
        edge_pair = pltpu.roll(rim, cy - 2 - 2 * place(v, r), 1)
        north = jnp.where(at_end, edge_pair, pltpu.roll(value, cy - 1, 1))
        south = jnp.where(at_start, edge_pair, pltpu.roll(value, 1, 1))
        return north, south

    def every(f):
        for v in range(variables):
            f(v)

    def rows_of(g, r):
        return pl.ds(g * span + r, GROUP, stride=cx)

    def convert_state(g):
        for v in range(variables):
            for r in range(cx):
                fld[0, v, g, r] = nat[v, rows_of(g, r), :]

    def pack_state(g, index):
        packed = jnp.zeros(shape, jnp.float32)
        for v in range(variables):
            for r in range(cx):
                packed = pack(packed, fld[index, v, g, r], v, r)
        return packed

    def start(copies):
        for copy in copies:
            copy.start()

    def over(a, b, f):
        lax.fori_loop(a, b, lambda g, c: (f(g), c)[1], 0)

    for g in order:
        state_in(g).wait()
        convert_state(g)
        if g == order[0]:
            pl.semaphore_wait(barrier, met)
        if g >= keep:
            @when(lends)
            def _():
                lend_state(g).start()

        packed = pack_state(g, 0)
        fold(0, g, packed)
        yp[0, g] = packed

        @when((k < end) & (g < hi))
        def _():
            start(field_halo(0, g, 0))

    @when(k > 0)
    def _():
        over(0, groups, lambda g: start(state_edges(g)))

    def convert_winds(n, g):
        for way in range(2):
            for j in range(GROUP):
                tile = wnat[2 * n + way, g * GROUP + j].astype(jnp.float32)
                for r in range(cx):
                    wr[2 * n + way, g, r, pl.ds(j, 1), :] = tile[r:r + 1]

    @when(k < end)
    def _():
        for n in range(steps):
            winds_in(n).wait()

            def one(i, n=n):
                g = lax.rem(i + keep, groups)
                convert_winds(n, g)
                if helping:
                    @when(lends & (g >= keep))
                    def _():
                        lend_winds(n, g).start()
            over(0, groups, one)

        @functools.partial(over, 0, groups)
        def _(g):
            packed = jnp.zeros(shape, jnp.float32)
            for r in range(cx):
                packed = pack(packed, wr[2 * steps - 1, g, r], 0, r)
            total = packed
            for v in range(1, variables):
                total = total + pltpu.roll(packed, 2 * place(v, 0), 1)
            yp[1, g] = total
            start(wind_edges(g))

    coupling_in.wait()

    if helping:
        @when(is_last)
        def _():
            @functools.partial(over, keep, groups)
            def _(g):
                lend_state(g).wait_recv()
                fold(0, g, pack_state(g, 1))
                start(field_halo(0, g, 1))

    def forward(n, g, final):
        if helping:
            @when(is_last)
            def _():
                lend_winds(n, g).wait_recv()
        receive(n, g)
        index = jnp.where(n == 0, sel, n + 1)
        rim = unfold(n, g)
        if final:
            for copy in state_edges(g):
                copy.wait_recv()

        def row(r):
            if r < 0:
                return [xr[n, 1, g, v] for v in range(variables)]
            if r == cx:
                return [xr[n, 0, g, v] for v in range(variables)]
            return [fld[index, v, g, r] for v in range(variables)]

        west, here = row(-1), row(0)
        packed = jnp.zeros(shape, jnp.float32)
        for r in range(cx):
            east = row(r + 1)
            u, w = wr[2 * n, g, r], wr[2 * n + 1, g, r]
            for v in range(variables):
                north, south = sides(here[v], rim, v, r)
                total = here[v] + u * (east[v] - west[v]) + w * (north - south)
                for b in range(variables):
                    total = total + cs[v, b] * here[b]
                fld[n + 2, v, g, r] = total
                if final and r == 0:
                    xs[0, 0, g, v] = xe[0, g, v] - total
                if final and r == cx - 1:
                    xs[0, 1, g, v] = xe[1, g, v] - total
                packed = pack(packed, total, v, r)
            west, here = here, east
        if final:
            fold(gap, g, ye[g] - packed)
            start(gap_halo(g))
            onward(g).start()
        else:
            fold(n + 1, g, packed)
            start(field_halo(n + 1, g, n + 2))

    @functools.partial(over, 0, steps - 1)
    def _(n):
        over(lo, hi, lambda g: forward(n, g, False))

    over(lo, hi, lambda g: forward(steps - 1, g, True))

    prec_in.wait()

    def stencil(g, row, rim, keeps):
        scale = []
        for v in range(variables):
            s = jnp.zeros(shape, jnp.float32)
            for j in range(GROUP):
                s = jnp.where(level == j, ps[v, g * GROUP + j], s)
            scale.append(s)
        west, here = row(-1), row(0)
        packed = jnp.zeros(shape, jnp.float32)
        for r in range(cx):
            east = row(r + 1)
            for v in range(variables):
                north, south = sides(here[v], rim, v, r)
                smooth = (1.0 + 4.0 * smooth_weight) * here[v] - smooth_weight * (
                    east[v] + west[v] + north + south)
                total = scale[v] * smooth
                wgt[v, g, r] = total
                if keeps:
                    packed = pack(packed, total, v, r)
                if keeps and r == 0:
                    xs[steps, 0, g, v] = xw[0, g] * total
                if keeps and r == cx - 1:
                    xs[steps, 1, g, v] = xw[1, g] * total
            west, here = here, east
        return packed

    def start_window(g):
        def row(r):
            if r < 0:
                return [xr[0, 1, g, v] for v in range(variables)]
            if r == cx:
                return [xr[0, 0, g, v] for v in range(variables)]
            return [fld[0, v, g, r] for v in range(variables)]
        stencil(g, row, unfold(0, g), False)

    def mismatch(g):
        receive(gap, g)
        onward(g).wait_recv()
        for copy in wind_edges(g):
            copy.wait_recv()

        def row(r):
            if r < 0:
                return [xr[gap, 1, g, v] for v in range(variables)]
            if r == cx:
                return [xr[gap, 0, g, v] for v in range(variables)]
            return [fld[0, v, g, r] - arrived[v, g, r] for v in range(variables)]
        fold(back0, g, yw[g] * stencil(g, row, unfold(gap, g), True))
        start(weighted_halo(g))
        back(g).start()

    @when(k > 0)
    def _():
        over(0, groups, mismatch)

    @when(is_first)
    def _():
        over(0, groups, start_window)

    def backward(i, g):
        n = steps - 1 - i
        slot = back0 + i
        first, final = i == 0, i == steps - 1
        if first:
            back(g).wait_recv()
        receive(slot, g)
        rim = unfold(slot, g)

        def row(r):
            if r < 0:
                return None, [xr[slot, 1, g, v] for v in range(variables)]
            if r == cx:
                return None, [xr[slot, 0, g, v] for v in range(variables)]
            u = wr[2 * n, g, r]
            values = [gf[i, v, g, r] for v in range(variables)]
            return values, [u * value for value in values]

        (_, west), (values, here) = row(-1), row(0)
        packed = jnp.zeros(shape, jnp.float32)
        for r in range(cx):
            values_east, east = row(r + 1)
            w = wr[2 * n + 1, g, r]
            if not final:
                u_next, w_next = wr[2 * n - 2, g, r], wr[2 * n - 1, g, r]
            for v in range(variables):
                north, south = sides(w * values[v], rim, v, r)
                total = values[v] + (west[v] - east[v]) + (south - north)
                for b in range(variables):
                    total = total + cs[b, v] * values[b]
                if final:
                    ret[v, g, r] = total
                    continue
                gf[i + 1, v, g, r] = total
                if r == 0:
                    xs[i + 1, 0, g, v] = u_next * total
                if r == cx - 1:
                    xs[i + 1, 1, g, v] = u_next * total
                packed = pack(packed, w_next * total, v, r)
            west, values, here = here, values_east, east
        if not final:
            fold(slot + 1, g, packed)
            start(flux_halo(i + 1, g))

    for i in range(steps - 1):
        over(back_lo, back_hi, functools.partial(backward, i))

    obs_in.wait()

    def finish(g, has_next):
        for v in range(variables):
            for r in range(cx):
                rows = rows_of(g, r)
                own = wgt[v, g, r] + onat[v, rows, :] * fld[0, v, g, r]
                out[v, rows, :] = own - ret[v, g, r] if has_next else own

    @functools.partial(over, back_lo, back_hi)
    def _(g):
        backward(steps - 1, g)

        @when(~is_last)
        def _():
            finish(g, True)
        if helping:
            @when(is_last)
            def _():
                give_back(g).start()

    @when(is_last)
    def _():
        @functools.partial(over, 0, groups)
        def _(g):
            finish(g, False)

    if helping:
        @when(lends)
        def _():
            @functools.partial(over, hold, groups)
            def _(g):
                give_back(g).wait_recv()
                finish(g, True)

    def sent(copies):
        for copy in copies:
            copy.wait_send()

    @functools.partial(over, lo, hi)
    def _(g):
        for n in range(steps):
            sent(field_halo(n, g, 0))
        sent(gap_halo(g))
        onward(g).wait_send()

    @functools.partial(over, back_lo, back_hi)
    def _(g):
        for i in range(1, steps):
            sent(flux_halo(i, g))

    @when(k > 0)
    def _():
        @functools.partial(over, 0, groups)
        def _(g):
            sent(weighted_halo(g))
            sent(state_edges(g))
            back(g).wait_send()

    @when(k < end)
    def _():
        over(0, groups, lambda g: sent(wind_edges(g)))

    if helping:
        @when(is_last)
        def _():
            over(hold, groups, lambda g: give_back(g).wait_send())

    if helping:
        @when(lends)
        def _():
            @functools.partial(over, keep, groups)
            def _(g):
                lend_state(g).wait_send()
                for n in range(steps):
                    lend_winds(n, g).wait_send()


def solution(mesh):
    windows, tiles = mesh.shape["win"], mesh.shape["tile"]

    def body(state, obs, trajectory, coupling, prec):
        block = state.shape[2:]
        variables, levels, cx, cy = block
        steps = trajectory.shape[2]
        groups = levels // GROUP
        keep, hold = (groups // 2, groups - groups // 4) if windows > 3 else (groups, groups)
        slots, half = 2 * steps + 1, GROUP // 2
        flat = (variables, levels * cx, cy)
        field = (variables, groups, cx, GROUP, cy)
        anywhere = pl.BlockSpec(memory_space=pltpu.HBM)
        f32 = jnp.float32
        result = pl.pallas_call(
            functools.partial(kernel, windows, tiles, keep, hold),
            out_shape=jax.ShapeDtypeStruct(flat, f32),
            in_specs=[anywhere] * 5,
            out_specs=pl.BlockSpec(memory_space=pltpu.VMEM),
            scratch_shapes=[
                pltpu.VMEM(flat, f32),
                pltpu.VMEM(flat, f32),
                pltpu.VMEM((2 * steps, levels, cx, cy), trajectory.dtype),
                pltpu.SMEM(coupling.shape, f32),
                pltpu.SMEM(prec.shape, f32),
                pltpu.VMEM((steps + 2,) + field, f32),
                pltpu.VMEM((2 * steps, groups, cx, GROUP, cy), f32),
                pltpu.VMEM(field, f32),
                pltpu.VMEM(field, f32),
                pltpu.VMEM((steps,) + field, f32),
                pltpu.VMEM(field, f32),
                pltpu.VMEM((steps + 1, 2, groups, variables, GROUP, cy), f32),
                pltpu.VMEM((slots, 2, groups, variables, GROUP, cy), f32),
                pltpu.VMEM((slots, 2, groups, half, cy), f32),
                pltpu.VMEM((slots, 2, groups, half, cy), f32),
                pltpu.VMEM((2, groups, GROUP, cy), f32),
                pltpu.VMEM((2, groups, variables, GROUP, cy), f32),
                pltpu.VMEM((groups, GROUP, cy), f32),
                pltpu.VMEM((2, groups, GROUP, cy), f32),
                pltpu.VMEM((groups, GROUP, cy), f32),
                pltpu.SemaphoreType.DMA((groups + steps + 3,)),
                pltpu.SemaphoreType.DMA((slots, 4, groups)),
                pltpu.SemaphoreType.DMA((slots, 4, groups)),
                pltpu.SemaphoreType.DMA((2, groups)),
                pltpu.SemaphoreType.DMA((2, groups)),
                pltpu.SemaphoreType.DMA((2 + steps, groups)),
                pltpu.SemaphoreType.DMA((2 + steps, groups)),
                pltpu.SemaphoreType.DMA((3, groups)),
                pltpu.SemaphoreType.DMA((3, groups)),
                pltpu.SemaphoreType.DMA((3, groups)),
                pltpu.SemaphoreType.DMA((3, groups)),
            ],
            compiler_params=pltpu.CompilerParams(
                collective_id=0, has_side_effects=True, vmem_limit_bytes=48 * 2**20),
        )(*[pltpu.with_memory_space_constraint(x, pltpu.HBM) for x in (
            state.reshape(flat), obs.reshape(flat),
            trajectory.reshape((2 * steps, levels, cx, cy)), coupling, prec)])
        return result.reshape((1, 1) + block)

    spec = P("win", "tile", None, None, None, None)
    return jax.shard_map(
        body, mesh=mesh,
        in_specs=(spec, spec, P("win", "tile", None, None, None, None, None), P(), P()),
        out_specs=spec, check_vma=False)
```

```python
import functools

import jax
import jax.numpy as jnp
from jax import lax
from jax.experimental import pallas as pl
from jax.experimental.pallas import tpu as pltpu
from jax.sharding import PartitionSpec as P

TY = 4
GROUP = 8

smooth_weight = 0.2


def kernel(windows, tiles, keep, hold, state, obs, winds, coupling, prec, out,
           nat, onat, wnat, cs, ps, fld, wr, arrived, wgt, gf, ret, xs, xr, ys, yr, yp, xe, ye, xw, yw,
           load, hsend, hrecv, wsend, wrecv, msend, mrecv, esend, erecv, fsend, frecv):
    steps, groups, cx, cy = wr.shape[0] // 2, wr.shape[1], wr.shape[2], wr.shape[4]
    variables = fld.shape[1]
    span = GROUP * cx
    end = windows - 1
    gap, back0 = steps, steps + 1
    half = GROUP // 2
    helping = keep < groups
    k = lax.axis_index("win")
    t = lax.axis_index("tile")
    before_x, after_x = lax.rem(t + tiles - TY, tiles), lax.rem(t + TY, tiles)
    before_y, after_y = lax.rem(t + tiles - 1, tiles), lax.rem(t + 1, tiles)
    around = (before_x, after_x, before_y, after_y)
    lender = end - 2
    is_first, is_last, lends = k == 0, k == end, k == lender
    lo, hi = jnp.where(is_last, keep, 0), jnp.where(lends, keep, groups)
    back_lo, back_hi = jnp.where(is_last, hold, 0), jnp.where(lends, hold, groups)
    sel = jnp.where(is_last, 1, 0)
    nxt = jnp.where(is_last, lender + 1, k + 1)

    def when(cond):
        return pl.when(cond)

    def part(g):
        return pl.ds(pl.multiple_of(g * span, span), span)

    def state_in(g):
        return pltpu.make_async_copy(state.at[:, part(g)], nat.at[:, part(g)], load.at[g])

    def winds_in(n):
        return pltpu.make_async_copy(winds.at[pl.ds(2 * n, 2)], wnat.at[pl.ds(2 * n, 2)], load.at[groups + n])

    obs_in = pltpu.make_async_copy(obs, onat, load.at[groups + steps])
    prec_in = pltpu.make_async_copy(prec, ps, load.at[groups + steps + 1])
    coupling_in = pltpu.make_async_copy(coupling, cs, load.at[groups + steps + 2])

    order = tuple(reversed(range(groups)))
    for g in order:
        state_in(g).start()
    coupling_in.start()

    @when(~is_last)
    def _():
        for n in range(steps):
            winds_in(n).start()
    prec_in.start()
    obs_in.start()

    barrier = pltpu.get_barrier_semaphore()

    def greet(win):
        pl.semaphore_signal(barrier, inc=1, device_id={"win": win})

    for other in around:
        pl.semaphore_signal(barrier, inc=1, device_id={"tile": other})

    @when(k < end)
    def _():
        greet(k + 1)

    @when(k > 0)
    def _():
        greet(k - 1)

    met = len(around) + jnp.where(k < end, 1, 0) + jnp.where(k > 0, 1, 0)
    if helping:
        @when(lends)
        def _():
            greet(end)

        @when(is_last)
        def _():
            greet(lender)
        met = met + jnp.where(lends | is_last, 1, 0)

    shape = (GROUP, cy)
    lane = lax.broadcasted_iota(jnp.int32, shape, 1)
    level = lax.broadcasted_iota(jnp.int32, shape, 0)
    pair, odd = lane // 2, lane % 2 == 1
    at_start, at_end = lane == 0, lane == cy - 1

    def halo(slot, g, win, low, high):
        made = []
        for side, to in enumerate((before_y, after_y)):
            made.append(pltpu.make_async_remote_copy(
                src_ref=ys.at[slot, side, g], dst_ref=yr.at[slot, side, g],
                send_sem=hsend.at[slot, side, g], recv_sem=hrecv.at[slot, side, g],
                device_id={"win": win, "tile": to}))
        for side, (to, rows) in enumerate(((before_x, low), (after_x, high))):
            made.append(pltpu.make_async_remote_copy(
                src_ref=rows, dst_ref=xr.at[slot, side, g],
                send_sem=hsend.at[slot, 2 + side, g], recv_sem=hrecv.at[slot, 2 + side, g],
                device_id={"win": win, "tile": to}))
        return made

    def field_halo(slot, g, index):
        return halo(slot, g, k, fld.at[index, :, g, 0], fld.at[index, :, g, cx - 1])

    def gap_halo(g):
        return halo(gap, g, nxt, xs.at[0, 0, g], xs.at[0, 1, g])

    def weighted_halo(g):
        return halo(back0, g, source(g, hold), xs.at[steps, 0, g], xs.at[steps, 1, g])

    def flux_halo(i, g):
        return halo(back0 + i, g, k, xs.at[i, 0, g], xs.at[i, 1, g])

    def receive(slot, g):
        for copy in halo(slot, g, k, xr.at[slot, 0, g], xr.at[slot, 1, g]):
            copy.wait_recv()

    def source(g, bound):
        return jnp.where((k == lender + 1) & (g >= bound), end, k - 1)

    def local_edges(pieces, sends, arrives, g, win):
        return [pltpu.make_async_remote_copy(
            src_ref=src, dst_ref=dst, send_sem=sends.at[i, g], recv_sem=arrives.at[i, g], device_id={"win": win})
            for i, (src, dst) in enumerate(pieces)]

    def state_edges(g):
        return local_edges((
            (fld.at[0, :, g, 0], xe.at[0, g]), (fld.at[0, :, g, cx - 1], xe.at[1, g]), (yp.at[0, g], ye.at[g]),
        ), esend, erecv, g, source(g, keep))

    def wind_edges(g):
        n = 2 * steps - 2
        return local_edges((
            (wr.at[n, g, 0], xw.at[0, g]), (wr.at[n, g, cx - 1], xw.at[1, g]), (yp.at[1, g], yw.at[g]),
        ), fsend, frecv, g, k + 1)

    def onward(g):
        return pltpu.make_async_remote_copy(
            src_ref=fld.at[steps + 1, :, g], dst_ref=arrived.at[:, g],
            send_sem=wsend.at[0, g], recv_sem=wrecv.at[0, g], device_id={"win": nxt})

    def back(g):
        return pltpu.make_async_remote_copy(
            src_ref=wgt.at[:, g], dst_ref=gf.at[0, :, g],
            send_sem=wsend.at[1, g], recv_sem=wrecv.at[1, g], device_id={"win": source(g, hold)})

    def lend_state(g):
        return pltpu.make_async_remote_copy(
            src_ref=fld.at[0, :, g], dst_ref=fld.at[1, :, g],
            send_sem=msend.at[0, g], recv_sem=mrecv.at[0, g], device_id={"win": end})

    def lend_winds(n, g):
        return pltpu.make_async_remote_copy(
            src_ref=wr.at[pl.ds(2 * n, 2), g], dst_ref=wr.at[pl.ds(2 * n, 2), g],
            send_sem=msend.at[2 + n, g], recv_sem=mrecv.at[2 + n, g], device_id={"win": end})

    def give_back(g):
        return pltpu.make_async_remote_copy(
            src_ref=ret.at[:, g], dst_ref=ret.at[:, g],
            send_sem=msend.at[1, g], recv_sem=mrecv.at[1, g], device_id={"win": lender})

    def place(v, r):
        return v * cx + r

    def pack(packed, value, v, r):
        p = place(v, r)
        return jnp.where(pair == p, pltpu.roll(value, 2 * p + 1, 1), packed)

    def fold(slot, g, packed):
        upper = pltpu.roll(pltpu.roll(packed, half, 0), 1, 1)
        ys[slot, 0, g] = jnp.where(odd, packed, upper)[:half]
        ys[slot, 1, g] = jnp.where(odd, upper, packed)[:half]

    def unfold(slot, g):
        north, south = [jnp.concatenate([yr[slot, side, g]] * 2, axis=0) for side in range(2)]
        north = jnp.where(level < half, north, pltpu.roll(north, cy - 1, 1))
        south = jnp.where(level < half, pltpu.roll(south, 2, 1), pltpu.roll(south, 1, 1))
        return jnp.where(odd, north, south)

    def sides(value, rim, v, r):
        edge_pair = pltpu.roll(rim, cy - 2 - 2 * place(v, r), 1)
        north = jnp.where(at_end, edge_pair, pltpu.roll(value, cy - 1, 1))
        south = jnp.where(at_start, edge_pair, pltpu.roll(value, 1, 1))
        return north, south

    def every(f):
        for v in range(variables):
            f(v)

    def rows_of(g, r):
        return pl.ds(g * span + r, GROUP, stride=cx)

    def convert_state(g):
        for v in range(variables):
            for r in range(cx):
                fld[0, v, g, r] = nat[v, rows_of(g, r), :]

    def pack_state(g, index):
        packed = jnp.zeros(shape, jnp.float32)
        for v in range(variables):
            for r in range(cx):
                packed = pack(packed, fld[index, v, g, r], v, r)
        return packed

    def start(copies):
        for copy in copies:
            copy.start()

    def over(a, b, f):
        lax.fori_loop(a, b, lambda i, c: (f(a + b - 1 - i), c)[1], 0)

    for g in order:
        state_in(g).wait()
        convert_state(g)
        if g == order[0]:
            pl.semaphore_wait(barrier, met)
        if g >= keep:
            @when(lends)
            def _():
                lend_state(g).start()

        packed = pack_state(g, 0)
        fold(0, g, packed)
        yp[0, g] = packed

        @when((k < end) & (g < hi))
        def _():
            start(field_halo(0, g, 0))

    @when(k > 0)
    def _():
        over(0, groups, lambda g: start(state_edges(g)))

    def convert_winds(n, g):
        for way in range(2):
            for j in range(GROUP):
                tile = wnat[2 * n + way, g * GROUP + j].astype(jnp.float32)
                for r in range(cx):
                    wr[2 * n + way, g, r, pl.ds(j, 1), :] = tile[r:r + 1]

    @when(k < end)
    def _():
        for n in range(steps):
            winds_in(n).wait()

            def one(i, n=n):
                g = lax.rem(i + keep, groups)
                convert_winds(n, g)
                if helping:
                    @when(lends & (g >= keep))
                    def _():
                        lend_winds(n, g).start()
            over(0, groups, one)

        @functools.partial(over, 0, groups)
        def _(g):
            packed = jnp.zeros(shape, jnp.float32)
            for r in range(cx):
                packed = pack(packed, wr[2 * steps - 1, g, r], 0, r)
            total = packed
            for v in range(1, variables):
                total = total + pltpu.roll(packed, 2 * place(v, 0), 1)
            yp[1, g] = total
            start(wind_edges(g))

    coupling_in.wait()

    if helping:
        @when(is_last)
        def _():
            @functools.partial(over, keep, groups)
            def _(g):
                lend_state(g).wait_recv()
                fold(0, g, pack_state(g, 1))
                start(field_halo(0, g, 1))

    def forward(n, g, final):
        if helping:
            @when(is_last)
            def _():
                lend_winds(n, g).wait_recv()
        receive(n, g)
        index = jnp.where(n == 0, sel, n + 1)
        rim = unfold(n, g)
        if final:
            for copy in state_edges(g):
                copy.wait_recv()

        def row(r):
            if r < 0:
                return [xr[n, 1, g, v] for v in range(variables)]
            if r == cx:
                return [xr[n, 0, g, v] for v in range(variables)]
            return [fld[index, v, g, r] for v in range(variables)]

        west, here = row(-1), row(0)
        packed = jnp.zeros(shape, jnp.float32)
        for r in range(cx):
            east = row(r + 1)
            u, w = wr[2 * n, g, r], wr[2 * n + 1, g, r]
            for v in range(variables):
                north, south = sides(here[v], rim, v, r)
                total = here[v] + u * (east[v] - west[v]) + w * (north - south)
                for b in range(variables):
                    total = total + cs[v, b] * here[b]
                fld[n + 2, v, g, r] = total
                if final and r == 0:
                    xs[0, 0, g, v] = xe[0, g, v] - total
                if final and r == cx - 1:
                    xs[0, 1, g, v] = xe[1, g, v] - total
                packed = pack(packed, total, v, r)
            west, here = here, east
        if final:
            fold(gap, g, ye[g] - packed)
            start(gap_halo(g))
            onward(g).start()
        else:
            fold(n + 1, g, packed)
            start(field_halo(n + 1, g, n + 2))

    def early_steps(n):
        over(lo, hi, lambda g: forward(n, g, False))

    lax.fori_loop(0, steps - 1, lambda n, c: (early_steps(n), c)[1], 0)
    over(lo, hi, lambda g: forward(steps - 1, g, True))

    prec_in.wait()

    def stencil(g, row, rim, keeps):
        scale = []
        for v in range(variables):
            s = jnp.zeros(shape, jnp.float32)
            for j in range(GROUP):
                s = jnp.where(level == j, ps[v, g * GROUP + j], s)
            scale.append(s)
        west, here = row(-1), row(0)
        packed = jnp.zeros(shape, jnp.float32)
        for r in range(cx):
            east = row(r + 1)
            for v in range(variables):
                north, south = sides(here[v], rim, v, r)
                smooth = (1.0 + 4.0 * smooth_weight) * here[v] - smooth_weight * (
                    east[v] + west[v] + north + south)
                total = scale[v] * smooth
                wgt[v, g, r] = total
                if keeps:
                    packed = pack(packed, total, v, r)
                if keeps and r == 0:
                    xs[steps, 0, g, v] = xw[0, g] * total
                if keeps and r == cx - 1:
                    xs[steps, 1, g, v] = xw[1, g] * total
            west, here = here, east
        return packed

    def start_window(g):
        def row(r):
            if r < 0:
                return [xr[0, 1, g, v] for v in range(variables)]
            if r == cx:
                return [xr[0, 0, g, v] for v in range(variables)]
            return [fld[0, v, g, r] for v in range(variables)]
        stencil(g, row, unfold(0, g), False)

    def mismatch(g):
        receive(gap, g)
        onward(g).wait_recv()
        for copy in wind_edges(g):
            copy.wait_recv()

        def row(r):
            if r < 0:
                return [xr[gap, 1, g, v] for v in range(variables)]
            if r == cx:
                return [xr[gap, 0, g, v] for v in range(variables)]
            return [fld[0, v, g, r] - arrived[v, g, r] for v in range(variables)]
        fold(back0, g, yw[g] * stencil(g, row, unfold(gap, g), True))
        start(weighted_halo(g))
        back(g).start()

    @when(k > 0)
    def _():
        over(0, groups, mismatch)

    @when(is_first)
    def _():
        over(0, groups, start_window)

    def backward(i, g):
        n = steps - 1 - i
        slot = back0 + i
        first, final = i == 0, i == steps - 1
        if first:
            back(g).wait_recv()
        receive(slot, g)
        rim = unfold(slot, g)

        def row(r):
            if r < 0:
                return None, [xr[slot, 1, g, v] for v in range(variables)]
            if r == cx:
                return None, [xr[slot, 0, g, v] for v in range(variables)]
            u = wr[2 * n, g, r]
            values = [gf[i, v, g, r] for v in range(variables)]
            return values, [u * value for value in values]

        (_, west), (values, here) = row(-1), row(0)
        packed = jnp.zeros(shape, jnp.float32)
        for r in range(cx):
            values_east, east = row(r + 1)
            w = wr[2 * n + 1, g, r]
            if not final:
                u_next, w_next = wr[2 * n - 2, g, r], wr[2 * n - 1, g, r]
            for v in range(variables):
                north, south = sides(w * values[v], rim, v, r)
                total = values[v] + (west[v] - east[v]) + (south - north)
                for b in range(variables):
                    total = total + cs[b, v] * values[b]
                if final:
                    ret[v, g, r] = total
                    continue
                gf[i + 1, v, g, r] = total
                if r == 0:
                    xs[i + 1, 0, g, v] = u_next * total
                if r == cx - 1:
                    xs[i + 1, 1, g, v] = u_next * total
                packed = pack(packed, w_next * total, v, r)
            west, values, here = here, values_east, east
        if not final:
            fold(slot + 1, g, packed)
            start(flux_halo(i + 1, g))

    for i in range(steps - 1):
        over(back_lo, back_hi, functools.partial(backward, i))

    obs_in.wait()

    def finish(g, has_next):
        for v in range(variables):
            for r in range(cx):
                rows = rows_of(g, r)
                own = wgt[v, g, r] + onat[v, rows, :] * fld[0, v, g, r]
                out[v, rows, :] = own - ret[v, g, r] if has_next else own

    @functools.partial(over, back_lo, back_hi)
    def _(g):
        backward(steps - 1, g)

        @when(~is_last)
        def _():
            finish(g, True)
        if helping:
            @when(is_last)
            def _():
                give_back(g).start()

    @when(is_last)
    def _():
        @functools.partial(over, 0, groups)
        def _(g):
            finish(g, False)

    if helping:
        @when(lends)
        def _():
            @functools.partial(over, hold, groups)
            def _(g):
                give_back(g).wait_recv()
                finish(g, True)

    def sent(copies):
        for copy in copies:
            copy.wait_send()

    @functools.partial(over, lo, hi)
    def _(g):
        for n in range(steps):
            sent(field_halo(n, g, 0))
        sent(gap_halo(g))
        onward(g).wait_send()

    @functools.partial(over, back_lo, back_hi)
    def _(g):
        for i in range(1, steps):
            sent(flux_halo(i, g))

    @when(k > 0)
    def _():
        @functools.partial(over, 0, groups)
        def _(g):
            sent(weighted_halo(g))
            sent(state_edges(g))
            back(g).wait_send()

    @when(k < end)
    def _():
        over(0, groups, lambda g: sent(wind_edges(g)))

    if helping:
        @when(is_last)
        def _():
            over(hold, groups, lambda g: give_back(g).wait_send())

    if helping:
        @when(lends)
        def _():
            @functools.partial(over, keep, groups)
            def _(g):
                lend_state(g).wait_send()
                for n in range(steps):
                    lend_winds(n, g).wait_send()


def solution(mesh):
    windows, tiles = mesh.shape["win"], mesh.shape["tile"]

    def body(state, obs, trajectory, coupling, prec):
        block = state.shape[2:]
        variables, levels, cx, cy = block
        steps = trajectory.shape[2]
        groups = levels // GROUP
        keep, hold = (groups // 2, groups - groups // 4) if windows > 3 else (groups, groups)
        slots, half = 2 * steps + 1, GROUP // 2
        flat = (variables, levels * cx, cy)
        field = (variables, groups, cx, GROUP, cy)
        anywhere = pl.BlockSpec(memory_space=pltpu.HBM)
        f32 = jnp.float32
        result = pl.pallas_call(
            functools.partial(kernel, windows, tiles, keep, hold),
            out_shape=jax.ShapeDtypeStruct(flat, f32),
            in_specs=[anywhere] * 5,
            out_specs=pl.BlockSpec(memory_space=pltpu.VMEM),
            scratch_shapes=[
                pltpu.VMEM(flat, f32),
                pltpu.VMEM(flat, f32),
                pltpu.VMEM((2 * steps, levels, cx, cy), trajectory.dtype),
                pltpu.SMEM(coupling.shape, f32),
                pltpu.SMEM(prec.shape, f32),
                pltpu.VMEM((steps + 2,) + field, f32),
                pltpu.VMEM((2 * steps, groups, cx, GROUP, cy), f32),
                pltpu.VMEM(field, f32),
                pltpu.VMEM(field, f32),
                pltpu.VMEM((steps,) + field, f32),
                pltpu.VMEM(field, f32),
                pltpu.VMEM((steps + 1, 2, groups, variables, GROUP, cy), f32),
                pltpu.VMEM((slots, 2, groups, variables, GROUP, cy), f32),
                pltpu.VMEM((slots, 2, groups, half, cy), f32),
                pltpu.VMEM((slots, 2, groups, half, cy), f32),
                pltpu.VMEM((2, groups, GROUP, cy), f32),
                pltpu.VMEM((2, groups, variables, GROUP, cy), f32),
                pltpu.VMEM((groups, GROUP, cy), f32),
                pltpu.VMEM((2, groups, GROUP, cy), f32),
                pltpu.VMEM((groups, GROUP, cy), f32),
                pltpu.SemaphoreType.DMA((groups + steps + 3,)),
                pltpu.SemaphoreType.DMA((slots, 4, groups)),
                pltpu.SemaphoreType.DMA((slots, 4, groups)),
                pltpu.SemaphoreType.DMA((2, groups)),
                pltpu.SemaphoreType.DMA((2, groups)),
                pltpu.SemaphoreType.DMA((2 + steps, groups)),
                pltpu.SemaphoreType.DMA((2 + steps, groups)),
                pltpu.SemaphoreType.DMA((3, groups)),
                pltpu.SemaphoreType.DMA((3, groups)),
                pltpu.SemaphoreType.DMA((3, groups)),
                pltpu.SemaphoreType.DMA((3, groups)),
            ],
            compiler_params=pltpu.CompilerParams(
                collective_id=0, has_side_effects=True, vmem_limit_bytes=48 * 2**20),
        )(*[pltpu.with_memory_space_constraint(x, pltpu.HBM) for x in (
            state.reshape(flat), obs.reshape(flat),
            trajectory.reshape((2 * steps, levels, cx, cy)), coupling, prec)])
        return result.reshape((1, 1) + block)

    spec = P("win", "tile", None, None, None, None)
    return jax.shard_map(
        body, mesh=mesh,
        in_specs=(spec, spec, P("win", "tile", None, None, None, None, None), P(), P()),
        out_specs=spec, check_vma=False)
```

```python
import functools

import jax
import jax.numpy as jnp
from jax import lax
from jax.experimental import pallas as pl
from jax.experimental.pallas import tpu as pltpu
from jax.sharding import PartitionSpec as P

TY = 4
GROUP = 8

smooth_weight = 0.2


def kernel(windows, tiles, keep, hold, state, obs, winds, coupling, prec, out,
           nat, onat, wnat, cs, ps, fld, wr, arrived, wgt, gf, ret, xs, xr, ys, yr, yp, xe, ye, xw, yw,
           load, hsend, hrecv, wsend, wrecv, msend, mrecv, esend, erecv, fsend, frecv):
    steps, groups, cx, cy = wr.shape[0] // 2, wr.shape[1], wr.shape[2], wr.shape[4]
    variables = fld.shape[1]
    span = GROUP * cx
    end = windows - 1
    gap, back0 = steps, steps + 1
    half = GROUP // 2
    helping = keep < groups
    k = lax.axis_index("win")
    t = lax.axis_index("tile")
    before_x, after_x = lax.rem(t + tiles - TY, tiles), lax.rem(t + TY, tiles)
    before_y, after_y = lax.rem(t + tiles - 1, tiles), lax.rem(t + 1, tiles)
    around = (before_x, after_x, before_y, after_y)
    lender = end - 2
    is_first, is_last, lends = k == 0, k == end, k == lender
    lo, hi = jnp.where(is_last, keep, 0), jnp.where(lends, keep, groups)
    back_lo, back_hi = jnp.where(is_last, hold, 0), jnp.where(lends, hold, groups)
    sel = jnp.where(is_last, 1, 0)
    nxt = jnp.where(is_last, lender + 1, k + 1)

    def when(cond):
        return pl.when(cond)

    def part(g):
        return pl.ds(pl.multiple_of(g * span, span), span)

    def state_in(g):
        return pltpu.make_async_copy(state.at[:, part(g)], nat.at[:, part(g)], load.at[g])

    def winds_in(n):
        return pltpu.make_async_copy(winds.at[pl.ds(2 * n, 2)], wnat.at[pl.ds(2 * n, 2)], load.at[groups + n])

    obs_in = pltpu.make_async_copy(obs, onat, load.at[groups + steps])
    prec_in = pltpu.make_async_copy(prec, ps, load.at[groups + steps + 1])
    coupling_in = pltpu.make_async_copy(coupling, cs, load.at[groups + steps + 2])

    order = tuple(reversed(range(groups)))
    for g in order:
        state_in(g).start()
    coupling_in.start()

    @when(~is_last)
    def _():
        for n in range(steps):
            winds_in(n).start()
    prec_in.start()
    obs_in.start()

    barrier = pltpu.get_barrier_semaphore()

    def greet(win):
        pl.semaphore_signal(barrier, inc=1, device_id={"win": win})

    for other in around:
        pl.semaphore_signal(barrier, inc=1, device_id={"tile": other})

    @when(k < end)
    def _():
        greet(k + 1)

    @when(k > 0)
    def _():
        greet(k - 1)

    met = len(around) + jnp.where(k < end, 1, 0) + jnp.where(k > 0, 1, 0)
    if helping:
        @when(lends)
        def _():
            greet(end)

        @when(is_last)
        def _():
            greet(lender)
        met = met + jnp.where(lends | is_last, 1, 0)

    shape = (GROUP, cy)
    lane = lax.broadcasted_iota(jnp.int32, shape, 1)
    level = lax.broadcasted_iota(jnp.int32, shape, 0)
    pair, odd = lane // 2, lane % 2 == 1
    at_start, at_end = lane == 0, lane == cy - 1

    def halo(slot, g, win, low, high):
        made = []
        for side, to in enumerate((before_y, after_y)):
            made.append(pltpu.make_async_remote_copy(
                src_ref=ys.at[slot, side, g], dst_ref=yr.at[slot, side, g],
                send_sem=hsend.at[slot, side, g], recv_sem=hrecv.at[slot, side, g],
                device_id={"win": win, "tile": to}))
        for side, (to, rows) in enumerate(((before_x, low), (after_x, high))):
            made.append(pltpu.make_async_remote_copy(
                src_ref=rows, dst_ref=xr.at[slot, side, g],
                send_sem=hsend.at[slot, 2 + side, g], recv_sem=hrecv.at[slot, 2 + side, g],
                device_id={"win": win, "tile": to}))
        return made

    def field_halo(slot, g, index):
        return halo(slot, g, k, fld.at[index, :, g, 0], fld.at[index, :, g, cx - 1])

    def gap_halo(g):
        return halo(gap, g, nxt, xs.at[0, 0, g], xs.at[0, 1, g])

    def weighted_halo(g):
        return halo(back0, g, source(g, hold), xs.at[steps, 0, g], xs.at[steps, 1, g])

    def flux_halo(i, g):
        return halo(back0 + i, g, k, xs.at[i, 0, g], xs.at[i, 1, g])

    def receive(slot, g):
        for copy in halo(slot, g, k, xr.at[slot, 0, g], xr.at[slot, 1, g]):
            copy.wait_recv()

    def source(g, bound):
        return jnp.where((k == lender + 1) & (g >= bound), end, k - 1)

    def local_edges(pieces, sends, arrives, g, win):
        return [pltpu.make_async_remote_copy(
            src_ref=src, dst_ref=dst, send_sem=sends.at[i, g], recv_sem=arrives.at[i, g], device_id={"win": win})
            for i, (src, dst) in enumerate(pieces)]

    def state_edges(g):
        return local_edges((
            (fld.at[0, :, g, 0], xe.at[0, g]), (fld.at[0, :, g, cx - 1], xe.at[1, g]), (yp.at[0, g], ye.at[g]),
        ), esend, erecv, g, source(g, keep))

    def wind_edges(g):
        n = 2 * steps - 2
        return local_edges((
            (wr.at[n, g, 0], xw.at[0, g]), (wr.at[n, g, cx - 1], xw.at[1, g]), (yp.at[1, g], yw.at[g]),
        ), fsend, frecv, g, k + 1)

    def onward(g):
        return pltpu.make_async_remote_copy(
            src_ref=fld.at[steps + 1, :, g], dst_ref=arrived.at[:, g],
            send_sem=wsend.at[0, g], recv_sem=wrecv.at[0, g], device_id={"win": nxt})

    def back(g):
        return pltpu.make_async_remote_copy(
            src_ref=wgt.at[:, g], dst_ref=gf.at[0, :, g],
            send_sem=wsend.at[1, g], recv_sem=wrecv.at[1, g], device_id={"win": source(g, hold)})

    def lend_state(g):
        return pltpu.make_async_remote_copy(
            src_ref=fld.at[0, :, g], dst_ref=fld.at[1, :, g],
            send_sem=msend.at[0, g], recv_sem=mrecv.at[0, g], device_id={"win": end})

    def lend_winds(n, g):
        return pltpu.make_async_remote_copy(
            src_ref=wr.at[pl.ds(2 * n, 2), g], dst_ref=wr.at[pl.ds(2 * n, 2), g],
            send_sem=msend.at[2 + n, g], recv_sem=mrecv.at[2 + n, g], device_id={"win": end})

    def give_back(g):
        return pltpu.make_async_remote_copy(
            src_ref=ret.at[:, g], dst_ref=ret.at[:, g],
            send_sem=msend.at[1, g], recv_sem=mrecv.at[1, g], device_id={"win": lender})

    def place(v, r):
        return v * cx + r

    def pack(packed, value, v, r):
        p = place(v, r)
        return jnp.where(pair == p, pltpu.roll(value, 2 * p + 1, 1), packed)

    def fold(slot, g, packed):
        upper = pltpu.roll(pltpu.roll(packed, half, 0), 1, 1)
        ys[slot, 0, g] = jnp.where(odd, packed, upper)[:half]
        ys[slot, 1, g] = jnp.where(odd, upper, packed)[:half]

    def unfold(slot, g):
        north, south = [jnp.concatenate([yr[slot, side, g]] * 2, axis=0) for side in range(2)]
        north = jnp.where(level < half, north, pltpu.roll(north, cy - 1, 1))
        south = jnp.where(level < half, pltpu.roll(south, 2, 1), pltpu.roll(south, 1, 1))
        return jnp.where(odd, north, south)

    def sides(value, rim, v, r):
        edge_pair = pltpu.roll(rim, cy - 2 - 2 * place(v, r), 1)
        north = jnp.where(at_end, edge_pair, pltpu.roll(value, cy - 1, 1))
        south = jnp.where(at_start, edge_pair, pltpu.roll(value, 1, 1))
        return north, south

    def every(f):
        for v in range(variables):
            f(v)

    def rows_of(g, r):
        return pl.ds(g * span + r, GROUP, stride=cx)

    def convert_state(g):
        for v in range(variables):
            for r in range(cx):
                fld[0, v, g, r] = nat[v, rows_of(g, r), :]

    def pack_state(g, index):
        packed = jnp.zeros(shape, jnp.float32)
        for v in range(variables):
            for r in range(cx):
                packed = pack(packed, fld[index, v, g, r], v, r)
        return packed

    def start(copies):
        for copy in copies:
            copy.start()

    def over(a, b, f):
        lax.fori_loop(a, b, lambda i, c: (f(a + b - 1 - i), c)[1], 0)

    for g in order:
        state_in(g).wait()
        convert_state(g)
        packed = pack_state(g, 0)
        fold(0, g, packed)
        yp[0, g] = packed
    pl.semaphore_wait(barrier, met)
    for g in order:
        if g >= keep:
            @when(lends)
            def _():
                lend_state(g).start()

    for part_of in (slice(0, 2), slice(2, 4)):
        for g in order:
            @when((k < end) & (g < hi))
            def _():
                start(field_halo(0, g, 0)[part_of])

    @when(k > 0)
    def _():
        over(0, groups, lambda g: start(state_edges(g)))

    def convert_winds(n, g):
        for way in range(2):
            for j in range(GROUP):
                tile = wnat[2 * n + way, g * GROUP + j].astype(jnp.float32)
                for r in range(cx):
                    wr[2 * n + way, g, r, pl.ds(j, 1), :] = tile[r:r + 1]

    @when(k < end)
    def _():
        for n in range(steps):
            winds_in(n).wait()

            def one(i, n=n):
                g = lax.rem(i + keep, groups)
                convert_winds(n, g)
                if helping:
                    @when(lends & (g >= keep))
                    def _():
                        lend_winds(n, g).start()
            over(0, groups, one)

        @functools.partial(over, 0, groups)
        def _(g):
            packed = jnp.zeros(shape, jnp.float32)
            for r in range(cx):
                packed = pack(packed, wr[2 * steps - 1, g, r], 0, r)
            total = packed
            for v in range(1, variables):
                total = total + pltpu.roll(packed, 2 * place(v, 0), 1)
            yp[1, g] = total
            start(wind_edges(g))

    coupling_in.wait()

    if helping:
        @when(is_last)
        def _():
            @functools.partial(over, keep, groups)
            def _(g):
                lend_state(g).wait_recv()
                fold(0, g, pack_state(g, 1))
                start(field_halo(0, g, 1))

    def forward(n, g, final):
        if helping:
            @when(is_last)
            def _():
                lend_winds(n, g).wait_recv()
        receive(n, g)
        index = jnp.where(n == 0, sel, n + 1)
        rim = unfold(n, g)
        if final:
            for copy in state_edges(g):
                copy.wait_recv()

        def row(r):
            if r < 0:
                return [xr[n, 1, g, v] for v in range(variables)]
            if r == cx:
                return [xr[n, 0, g, v] for v in range(variables)]
            return [fld[index, v, g, r] for v in range(variables)]

        west, here = row(-1), row(0)
        packed = jnp.zeros(shape, jnp.float32)
        for r in range(cx):
            east = row(r + 1)
            u, w = wr[2 * n, g, r], wr[2 * n + 1, g, r]
            for v in range(variables):
                north, south = sides(here[v], rim, v, r)
                total = here[v] + u * (east[v] - west[v]) + w * (north - south)
                for b in range(variables):
                    total = total + cs[v, b] * here[b]
                fld[n + 2, v, g, r] = total
                if final and r == 0:
                    xs[0, 0, g, v] = xe[0, g, v] - total
                if final and r == cx - 1:
                    xs[0, 1, g, v] = xe[1, g, v] - total
                packed = pack(packed, total, v, r)
            west, here = here, east
        if final:
            fold(gap, g, ye[g] - packed)
            start(gap_halo(g))
            onward(g).start()
        else:
            fold(n + 1, g, packed)
            start(field_halo(n + 1, g, n + 2))

    def early_steps(n):
        over(lo, hi, lambda g: forward(n, g, False))

    lax.fori_loop(0, steps - 1, lambda n, c: (early_steps(n), c)[1], 0)
    over(lo, hi, lambda g: forward(steps - 1, g, True))

    prec_in.wait()

    def stencil(g, row, rim, keeps):
        scale = []
        for v in range(variables):
            s = jnp.zeros(shape, jnp.float32)
            for j in range(GROUP):
                s = jnp.where(level == j, ps[v, g * GROUP + j], s)
            scale.append(s)
        west, here = row(-1), row(0)
        packed = jnp.zeros(shape, jnp.float32)
        for r in range(cx):
            east = row(r + 1)
            for v in range(variables):
                north, south = sides(here[v], rim, v, r)
                smooth = (1.0 + 4.0 * smooth_weight) * here[v] - smooth_weight * (
                    east[v] + west[v] + north + south)
                total = scale[v] * smooth
                wgt[v, g, r] = total
                if keeps:
                    packed = pack(packed, total, v, r)
                if keeps and r == 0:
                    xs[steps, 0, g, v] = xw[0, g] * total
                if keeps and r == cx - 1:
                    xs[steps, 1, g, v] = xw[1, g] * total
            west, here = here, east
        return packed

    def start_window(g):
        def row(r):
            if r < 0:
                return [xr[0, 1, g, v] for v in range(variables)]
            if r == cx:
                return [xr[0, 0, g, v] for v in range(variables)]
            return [fld[0, v, g, r] for v in range(variables)]
        stencil(g, row, unfold(0, g), False)

    def mismatch(g):
        receive(gap, g)
        onward(g).wait_recv()
        for copy in wind_edges(g):
            copy.wait_recv()

        def row(r):
            if r < 0:
                return [xr[gap, 1, g, v] for v in range(variables)]
            if r == cx:
                return [xr[gap, 0, g, v] for v in range(variables)]
            return [fld[0, v, g, r] - arrived[v, g, r] for v in range(variables)]
        fold(back0, g, yw[g] * stencil(g, row, unfold(gap, g), True))
        start(weighted_halo(g))
        back(g).start()

    @when(k > 0)
    def _():
        over(0, groups, mismatch)

    @when(is_first)
    def _():
        over(0, groups, start_window)

    def backward(i, g):
        n = steps - 1 - i
        slot = back0 + i
        first, final = i == 0, i == steps - 1
        if first:
            back(g).wait_recv()
        receive(slot, g)
        rim = unfold(slot, g)

        def row(r):
            if r < 0:
                return None, [xr[slot, 1, g, v] for v in range(variables)]
            if r == cx:
                return None, [xr[slot, 0, g, v] for v in range(variables)]
            u = wr[2 * n, g, r]
            values = [gf[i, v, g, r] for v in range(variables)]
            return values, [u * value for value in values]

        (_, west), (values, here) = row(-1), row(0)
        packed = jnp.zeros(shape, jnp.float32)
        for r in range(cx):
            values_east, east = row(r + 1)
            w = wr[2 * n + 1, g, r]
            if not final:
                u_next, w_next = wr[2 * n - 2, g, r], wr[2 * n - 1, g, r]
            for v in range(variables):
                north, south = sides(w * values[v], rim, v, r)
                total = values[v] + (west[v] - east[v]) + (south - north)
                for b in range(variables):
                    total = total + cs[b, v] * values[b]
                if final:
                    ret[v, g, r] = total
                    continue
                gf[i + 1, v, g, r] = total
                if r == 0:
                    xs[i + 1, 0, g, v] = u_next * total
                if r == cx - 1:
                    xs[i + 1, 1, g, v] = u_next * total
                packed = pack(packed, w_next * total, v, r)
            west, values, here = here, values_east, east
        if not final:
            fold(slot + 1, g, packed)
            start(flux_halo(i + 1, g))

    for i in range(steps - 1):
        over(back_lo, back_hi, functools.partial(backward, i))

    obs_in.wait()

    def finish(g, has_next):
        for v in range(variables):
            for r in range(cx):
                rows = rows_of(g, r)
                own = wgt[v, g, r] + onat[v, rows, :] * fld[0, v, g, r]
                out[v, rows, :] = own - ret[v, g, r] if has_next else own

    @functools.partial(over, back_lo, back_hi)
    def _(g):
        backward(steps - 1, g)

        @when(~is_last)
        def _():
            finish(g, True)
        if helping:
            @when(is_last)
            def _():
                give_back(g).start()

    @when(is_last)
    def _():
        @functools.partial(over, 0, groups)
        def _(g):
            finish(g, False)

    if helping:
        @when(lends)
        def _():
            @functools.partial(over, hold, groups)
            def _(g):
                give_back(g).wait_recv()
                finish(g, True)

    def sent(copies):
        for copy in copies:
            copy.wait_send()

    @functools.partial(over, lo, hi)
    def _(g):
        for n in range(steps):
            sent(field_halo(n, g, 0))
        sent(gap_halo(g))
        onward(g).wait_send()

    @functools.partial(over, back_lo, back_hi)
    def _(g):
        for i in range(1, steps):
            sent(flux_halo(i, g))

    @when(k > 0)
    def _():
        @functools.partial(over, 0, groups)
        def _(g):
            sent(weighted_halo(g))
            sent(state_edges(g))
            back(g).wait_send()

    @when(k < end)
    def _():
        over(0, groups, lambda g: sent(wind_edges(g)))

    if helping:
        @when(is_last)
        def _():
            over(hold, groups, lambda g: give_back(g).wait_send())

    if helping:
        @when(lends)
        def _():
            @functools.partial(over, keep, groups)
            def _(g):
                lend_state(g).wait_send()
                for n in range(steps):
                    lend_winds(n, g).wait_send()


def solution(mesh):
    windows, tiles = mesh.shape["win"], mesh.shape["tile"]

    def body(state, obs, trajectory, coupling, prec):
        block = state.shape[2:]
        variables, levels, cx, cy = block
        steps = trajectory.shape[2]
        groups = levels // GROUP
        keep, hold = (groups // 2, groups - groups // 4) if windows > 3 else (groups, groups)
        slots, half = 2 * steps + 1, GROUP // 2
        flat = (variables, levels * cx, cy)
        field = (variables, groups, cx, GROUP, cy)
        anywhere = pl.BlockSpec(memory_space=pltpu.HBM)
        f32 = jnp.float32
        result = pl.pallas_call(
            functools.partial(kernel, windows, tiles, keep, hold),
            out_shape=jax.ShapeDtypeStruct(flat, f32),
            in_specs=[anywhere] * 5,
            out_specs=pl.BlockSpec(memory_space=pltpu.VMEM),
            scratch_shapes=[
                pltpu.VMEM(flat, f32),
                pltpu.VMEM(flat, f32),
                pltpu.VMEM((2 * steps, levels, cx, cy), trajectory.dtype),
                pltpu.SMEM(coupling.shape, f32),
                pltpu.SMEM(prec.shape, f32),
                pltpu.VMEM((steps + 2,) + field, f32),
                pltpu.VMEM((2 * steps, groups, cx, GROUP, cy), f32),
                pltpu.VMEM(field, f32),
                pltpu.VMEM(field, f32),
                pltpu.VMEM((steps,) + field, f32),
                pltpu.VMEM(field, f32),
                pltpu.VMEM((steps + 1, 2, groups, variables, GROUP, cy), f32),
                pltpu.VMEM((slots, 2, groups, variables, GROUP, cy), f32),
                pltpu.VMEM((slots, 2, groups, half, cy), f32),
                pltpu.VMEM((slots, 2, groups, half, cy), f32),
                pltpu.VMEM((2, groups, GROUP, cy), f32),
                pltpu.VMEM((2, groups, variables, GROUP, cy), f32),
                pltpu.VMEM((groups, GROUP, cy), f32),
                pltpu.VMEM((2, groups, GROUP, cy), f32),
                pltpu.VMEM((groups, GROUP, cy), f32),
                pltpu.SemaphoreType.DMA((groups + steps + 3,)),
                pltpu.SemaphoreType.DMA((slots, 4, groups)),
                pltpu.SemaphoreType.DMA((slots, 4, groups)),
                pltpu.SemaphoreType.DMA((2, groups)),
                pltpu.SemaphoreType.DMA((2, groups)),
                pltpu.SemaphoreType.DMA((2 + steps, groups)),
                pltpu.SemaphoreType.DMA((2 + steps, groups)),
                pltpu.SemaphoreType.DMA((3, groups)),
                pltpu.SemaphoreType.DMA((3, groups)),
                pltpu.SemaphoreType.DMA((3, groups)),
                pltpu.SemaphoreType.DMA((3, groups)),
            ],
            compiler_params=pltpu.CompilerParams(
                collective_id=0, has_side_effects=True, vmem_limit_bytes=48 * 2**20),
        )(*[pltpu.with_memory_space_constraint(x, pltpu.HBM) for x in (
            state.reshape(flat), obs.reshape(flat),
            trajectory.reshape((2 * steps, levels, cx, cy)), coupling, prec)])
        return result.reshape((1, 1) + block)

    spec = P("win", "tile", None, None, None, None)
    return jax.shard_map(
        body, mesh=mesh,
        in_specs=(spec, spec, P("win", "tile", None, None, None, None, None), P(), P()),
        out_specs=spec, check_vma=False)
```

```python
import functools

import jax
import jax.numpy as jnp
from jax import lax
from jax.experimental import pallas as pl
from jax.experimental.pallas import tpu as pltpu
from jax.sharding import PartitionSpec as P

TY = 4
GROUP = 8

smooth_weight = 0.2


def kernel(windows, tiles, keep, hold, state, obs, winds, coupling, prec, out,
           nat, onat, wnat, cs, ps, fld, wr, arrived, wgt, gf, ret, xs, xr, ys, yr, yp, xe, ye, xw, yw,
           load, hsend, hrecv, wsend, wrecv, msend, mrecv, esend, erecv, fsend, frecv):
    steps, groups, cx, cy = wr.shape[0] // 2, wr.shape[1], wr.shape[2], wr.shape[4]
    variables = fld.shape[1]
    span = GROUP * cx
    end = windows - 1
    gap, back0 = steps, steps + 1
    half = GROUP // 2
    helping = keep < groups
    k = lax.axis_index("win")
    t = lax.axis_index("tile")
    before_x, after_x = lax.rem(t + tiles - TY, tiles), lax.rem(t + TY, tiles)
    before_y, after_y = lax.rem(t + tiles - 1, tiles), lax.rem(t + 1, tiles)
    around = (before_x, after_x, before_y, after_y)
    lender = end - 2
    is_first, is_last, lends = k == 0, k == end, k == lender
    lo, hi = jnp.where(is_last, keep, 0), jnp.where(lends, keep, groups)
    back_lo, back_hi = jnp.where(is_last, hold, 0), jnp.where(lends, hold, groups)
    sel = jnp.where(is_last, 1, 0)
    nxt = jnp.where(is_last, lender + 1, k + 1)

    def when(cond):
        return pl.when(cond)

    def part(g):
        return pl.ds(pl.multiple_of(g * span, span), span)

    def state_in(g):
        return pltpu.make_async_copy(state.at[:, part(g)], nat.at[:, part(g)], load.at[g])

    def winds_in(n):
        return pltpu.make_async_copy(winds.at[pl.ds(2 * n, 2)], wnat.at[pl.ds(2 * n, 2)], load.at[groups + n])

    obs_in = pltpu.make_async_copy(obs, onat, load.at[groups + steps])
    prec_in = pltpu.make_async_copy(prec, ps, load.at[groups + steps + 1])
    coupling_in = pltpu.make_async_copy(coupling, cs, load.at[groups + steps + 2])

    order = tuple(reversed(range(groups)))
    for g in order:
        state_in(g).start()
    coupling_in.start()

    @when(~is_last)
    def _():
        for n in range(steps):
            winds_in(n).start()
    prec_in.start()
    obs_in.start()

    barrier = pltpu.get_barrier_semaphore()

    def greet(win):
        pl.semaphore_signal(barrier, inc=1, device_id={"win": win})

    for other in around:
        pl.semaphore_signal(barrier, inc=1, device_id={"tile": other})

    @when(k < end)
    def _():
        greet(k + 1)

    @when(k > 0)
    def _():
        greet(k - 1)

    met = len(around) + jnp.where(k < end, 1, 0) + jnp.where(k > 0, 1, 0)
    if helping:
        @when(lends)
        def _():
            greet(end)

        @when(is_last)
        def _():
            greet(lender)
        met = met + jnp.where(lends | is_last, 1, 0)

    shape = (GROUP, cy)
    lane = lax.broadcasted_iota(jnp.int32, shape, 1)
    level = lax.broadcasted_iota(jnp.int32, shape, 0)
    pair, odd = lane // 2, lane % 2 == 1
    at_start, at_end = lane == 0, lane == cy - 1

    def halo(slot, g, win, low, high):
        made = []
        for side, to in enumerate((before_y, after_y)):
            made.append(pltpu.make_async_remote_copy(
                src_ref=ys.at[slot, side, g], dst_ref=yr.at[slot, side, g],
                send_sem=hsend.at[slot, side, g], recv_sem=hrecv.at[slot, side, g],
                device_id={"win": win, "tile": to}))
        for side, (to, rows) in enumerate(((before_x, low), (after_x, high))):
            made.append(pltpu.make_async_remote_copy(
                src_ref=rows, dst_ref=xr.at[slot, side, g],
                send_sem=hsend.at[slot, 2 + side, g], recv_sem=hrecv.at[slot, 2 + side, g],
                device_id={"win": win, "tile": to}))
        return made

    def field_halo(slot, g, index):
        return halo(slot, g, k, fld.at[index, :, g, 0], fld.at[index, :, g, cx - 1])

    def gap_halo(g):
        return halo(gap, g, nxt, xs.at[0, 0, g], xs.at[0, 1, g])

    def weighted_halo(g):
        return halo(back0, g, source(g, hold), xs.at[steps, 0, g], xs.at[steps, 1, g])

    def flux_halo(i, g):
        return halo(back0 + i, g, k, xs.at[i, 0, g], xs.at[i, 1, g])

    def receive(slot, g):
        for copy in halo(slot, g, k, xr.at[slot, 0, g], xr.at[slot, 1, g]):
            copy.wait_recv()

    def source(g, bound):
        return jnp.where((k == lender + 1) & (g >= bound), end, k - 1)

    def local_edges(pieces, sends, arrives, g, win):
        return [pltpu.make_async_remote_copy(
            src_ref=src, dst_ref=dst, send_sem=sends.at[i, g], recv_sem=arrives.at[i, g], device_id={"win": win})
            for i, (src, dst) in enumerate(pieces)]

    def state_edges(g):
        return local_edges((
            (fld.at[0, :, g, 0], xe.at[0, g]), (fld.at[0, :, g, cx - 1], xe.at[1, g]), (yp.at[0, g], ye.at[g]),
        ), esend, erecv, g, source(g, keep))

    def wind_edges(g):
        n = 2 * steps - 2
        return local_edges((
            (wr.at[n, g, 0], xw.at[0, g]), (wr.at[n, g, cx - 1], xw.at[1, g]), (yp.at[1, g], yw.at[g]),
        ), fsend, frecv, g, k + 1)

    def onward(g):
        return pltpu.make_async_remote_copy(
            src_ref=fld.at[steps + 1, :, g], dst_ref=arrived.at[:, g],
            send_sem=wsend.at[0, g], recv_sem=wrecv.at[0, g], device_id={"win": nxt})

    def back(g):
        return pltpu.make_async_remote_copy(
            src_ref=wgt.at[:, g], dst_ref=gf.at[0, :, g],
            send_sem=wsend.at[1, g], recv_sem=wrecv.at[1, g], device_id={"win": source(g, hold)})

    def lend_state(g):
        return pltpu.make_async_remote_copy(
            src_ref=fld.at[0, :, g], dst_ref=fld.at[1, :, g],
            send_sem=msend.at[0, g], recv_sem=mrecv.at[0, g], device_id={"win": end})

    def lend_winds(n, g):
        return pltpu.make_async_remote_copy(
            src_ref=wr.at[pl.ds(2 * n, 2), g], dst_ref=wr.at[pl.ds(2 * n, 2), g],
            send_sem=msend.at[2 + n, g], recv_sem=mrecv.at[2 + n, g], device_id={"win": end})

    def give_back(g):
        return pltpu.make_async_remote_copy(
            src_ref=ret.at[:, g], dst_ref=ret.at[:, g],
            send_sem=msend.at[1, g], recv_sem=mrecv.at[1, g], device_id={"win": lender})

    def place(v, r):
        return v * cx + r

    def pack(packed, value, v, r):
        p = place(v, r)
        return jnp.where(pair == p, pltpu.roll(value, 2 * p + 1, 1), packed)

    def fold(slot, g, packed):
        upper = pltpu.roll(pltpu.roll(packed, half, 0), 1, 1)
        ys[slot, 0, g] = jnp.where(odd, packed, upper)[:half]
        ys[slot, 1, g] = jnp.where(odd, upper, packed)[:half]

    def unfold(slot, g):
        north, south = [jnp.concatenate([yr[slot, side, g]] * 2, axis=0) for side in range(2)]
        north = jnp.where(level < half, north, pltpu.roll(north, cy - 1, 1))
        south = jnp.where(level < half, pltpu.roll(south, 2, 1), pltpu.roll(south, 1, 1))
        return jnp.where(odd, north, south)

    def sides(value, rim, v, r):
        edge_pair = pltpu.roll(rim, cy - 2 - 2 * place(v, r), 1)
        north = jnp.where(at_end, edge_pair, pltpu.roll(value, cy - 1, 1))
        south = jnp.where(at_start, edge_pair, pltpu.roll(value, 1, 1))
        return north, south

    def every(f):
        for v in range(variables):
            f(v)

    def rows_of(g, r):
        return pl.ds(g * span + r, GROUP, stride=cx)

    def convert_state(g):
        for v in range(variables):
            for r in range(cx):
                fld[0, v, g, r] = nat[v, rows_of(g, r), :]

    def pack_state(g, index):
        packed = jnp.zeros(shape, jnp.float32)
        for v in range(variables):
            for r in range(cx):
                packed = pack(packed, fld[index, v, g, r], v, r)
        return packed

    def start(copies):
        for copy in copies:
            copy.start()

    def over(a, b, f):
        lax.fori_loop(a, b, lambda i, c: (f(a + b - 1 - i), c)[1], 0)

    for g in order:
        state_in(g).wait()
        convert_state(g)
        packed = pack_state(g, 0)
        fold(0, g, packed)
        yp[0, g] = packed
    pl.semaphore_wait(barrier, met)
    for g in order:
        if g >= keep:
            @when(lends)
            def _():
                lend_state(g).start()

    for part_of in (slice(0, 2), slice(2, 4)):
        for g in order:
            @when((k < end) & (g < hi))
            def _():
                start(field_halo(0, g, 0)[part_of])

    @when(k > 0)
    def _():
        over(0, groups, lambda g: start(state_edges(g)))

    def convert_winds(n, g):
        for way in range(2):
            for j in range(GROUP):
                tile = wnat[2 * n + way, g * GROUP + j].astype(jnp.float32)
                for r in range(cx):
                    wr[2 * n + way, g, r, pl.ds(j, 1), :] = tile[r:r + 1]

    @when(k < end)
    def _():
        for n in range(steps):
            winds_in(n).wait()

            def one(i, n=n):
                g = lax.rem(i + keep, groups)
                convert_winds(n, g)
                if helping:
                    @when(lends & (g >= keep))
                    def _():
                        lend_winds(n, g).start()
            over(0, groups, one)

        @functools.partial(over, 0, groups)
        def _(g):
            packed = jnp.zeros(shape, jnp.float32)
            for r in range(cx):
                packed = pack(packed, wr[2 * steps - 1, g, r], 0, r)
            total = packed
            for v in range(1, variables):
                total = total + pltpu.roll(packed, 2 * place(v, 0), 1)
            yp[1, g] = total
            start(wind_edges(g))

    coupling_in.wait()

    if helping:
        @when(is_last)
        def _():
            @functools.partial(over, keep, groups)
            def _(g):
                lend_state(g).wait_recv()
                fold(0, g, pack_state(g, 1))
                start(field_halo(0, g, 1))

    def forward(n, g, final):
        if helping:
            @when(is_last)
            def _():
                lend_winds(n, g).wait_recv()
        receive(n, g)
        index = jnp.where(n == 0, sel, n + 1)
        rim = unfold(n, g)
        if final:
            for copy in state_edges(g):
                copy.wait_recv()

        def row(r):
            if r < 0:
                return [xr[n, 1, g, v] for v in range(variables)]
            if r == cx:
                return [xr[n, 0, g, v] for v in range(variables)]
            return [fld[index, v, g, r] for v in range(variables)]

        west, here = row(-1), row(0)
        packed = jnp.zeros(shape, jnp.float32)
        for r in range(cx):
            east = row(r + 1)
            u, w = wr[2 * n, g, r], wr[2 * n + 1, g, r]
            for v in range(variables):
                north, south = sides(here[v], rim, v, r)
                total = here[v] + u * (east[v] - west[v]) + w * (north - south)
                for b in range(variables):
                    total = total + cs[v, b] * here[b]
                fld[n + 2, v, g, r] = total
                if final and r == 0:
                    xs[0, 0, g, v] = xe[0, g, v] - total
                if final and r == cx - 1:
                    xs[0, 1, g, v] = xe[1, g, v] - total
                packed = pack(packed, total, v, r)
            west, here = here, east
        if final:
            fold(gap, g, ye[g] - packed)
            start(gap_halo(g))
            onward(g).start()
        else:
            fold(n + 1, g, packed)
            start(field_halo(n + 1, g, n + 2))

    def early_steps(n):
        over(lo, hi, lambda g: forward(n, g, False))

    lax.fori_loop(0, steps - 1, lambda n, c: (early_steps(n), c)[1], 0)
    over(lo, hi, lambda g: forward(steps - 1, g, True))

    prec_in.wait()

    def stencil(g, row, rim, keeps):
        scale = []
        for v in range(variables):
            s = jnp.zeros(shape, jnp.float32)
            for j in range(GROUP):
                s = jnp.where(level == j, ps[v, g * GROUP + j], s)
            scale.append(s)
        west, here = row(-1), row(0)
        packed = jnp.zeros(shape, jnp.float32)
        for r in range(cx):
            east = row(r + 1)
            for v in range(variables):
                north, south = sides(here[v], rim, v, r)
                smooth = (1.0 + 4.0 * smooth_weight) * here[v] - smooth_weight * (
                    east[v] + west[v] + north + south)
                total = scale[v] * smooth
                wgt[v, g, r] = total
                if keeps:
                    packed = pack(packed, total, v, r)
                if keeps and r == 0:
                    xs[steps, 0, g, v] = xw[0, g] * total
                if keeps and r == cx - 1:
                    xs[steps, 1, g, v] = xw[1, g] * total
            west, here = here, east
        return packed

    def start_window(g):
        def row(r):
            if r < 0:
                return [xr[0, 1, g, v] for v in range(variables)]
            if r == cx:
                return [xr[0, 0, g, v] for v in range(variables)]
            return [fld[0, v, g, r] for v in range(variables)]
        stencil(g, row, unfold(0, g), False)

    def mismatch(g):
        receive(gap, g)
        onward(g).wait_recv()
        for copy in wind_edges(g):
            copy.wait_recv()

        def row(r):
            if r < 0:
                return [xr[gap, 1, g, v] for v in range(variables)]
            if r == cx:
                return [xr[gap, 0, g, v] for v in range(variables)]
            return [fld[0, v, g, r] - arrived[v, g, r] for v in range(variables)]
        fold(back0, g, yw[g] * stencil(g, row, unfold(gap, g), True))
        start(weighted_halo(g))
        back(g).start()

    @when(k > 0)
    def _():
        over(0, groups, lambda i: mismatch(jnp.where((k == 2) & (i < hold), lax.rem(i + keep, hold), i)))

    @when(is_first)
    def _():
        over(0, groups, start_window)

    def backward(i, g):
        n = steps - 1 - i
        slot = back0 + i
        first, final = i == 0, i == steps - 1
        if first:
            back(g).wait_recv()
        receive(slot, g)
        rim = unfold(slot, g)

        def row(r):
            if r < 0:
                return None, [xr[slot, 1, g, v] for v in range(variables)]
            if r == cx:
                return None, [xr[slot, 0, g, v] for v in range(variables)]
            u = wr[2 * n, g, r]
            values = [gf[i, v, g, r] for v in range(variables)]
            return values, [u * value for value in values]

        (_, west), (values, here) = row(-1), row(0)
        packed = jnp.zeros(shape, jnp.float32)
        for r in range(cx):
            values_east, east = row(r + 1)
            w = wr[2 * n + 1, g, r]
            if not final:
                u_next, w_next = wr[2 * n - 2, g, r], wr[2 * n - 1, g, r]
            for v in range(variables):
                north, south = sides(w * values[v], rim, v, r)
                total = values[v] + (west[v] - east[v]) + (south - north)
                for b in range(variables):
                    total = total + cs[b, v] * values[b]
                if final:
                    ret[v, g, r] = total
                    continue
                gf[i + 1, v, g, r] = total
                if r == 0:
                    xs[i + 1, 0, g, v] = u_next * total
                if r == cx - 1:
                    xs[i + 1, 1, g, v] = u_next * total
                packed = pack(packed, w_next * total, v, r)
            west, values, here = here, values_east, east
        if not final:
            fold(slot + 1, g, packed)
            start(flux_halo(i + 1, g))

    for i in range(steps - 1):
        over(back_lo, back_hi, lambda j, i=i: backward(i, jnp.where(k == 1, lax.rem(j + keep, hold), j)))

    def sent(copies):
        for copy in copies:
            copy.wait_send()

    @functools.partial(over, lo, hi)
    def _(g):
        for n in range(steps):
            sent(field_halo(n, g, 0))
        sent(gap_halo(g))
        onward(g).wait_send()

    @when(k > 0)
    def _():
        @functools.partial(over, 0, groups)
        def _(g):
            sent(weighted_halo(g))
            sent(state_edges(g))
            back(g).wait_send()

    @when(k < end)
    def _():
        over(0, groups, lambda g: sent(wind_edges(g)))

    if helping:
        @when(lends)
        def _():
            @functools.partial(over, keep, groups)
            def _(g):
                lend_state(g).wait_send()
                for n in range(steps):
                    lend_winds(n, g).wait_send()

    obs_in.wait()

    def finish(g, has_next):
        for v in range(variables):
            for r in range(cx):
                rows = rows_of(g, r)
                own = wgt[v, g, r] + onat[v, rows, :] * fld[0, v, g, r]
                out[v, rows, :] = own - ret[v, g, r] if has_next else own

    @functools.partial(over, back_lo, back_hi)
    def _(j):
        g = jnp.where(k == 1, lax.rem(j + keep, hold), j)
        backward(steps - 1, g)

        @when(~is_last)
        def _():
            finish(g, True)
        if helping:
            @when(is_last)
            def _():
                give_back(g).start()

    @when(is_last)
    def _():
        @functools.partial(over, 0, groups)
        def _(g):
            finish(g, False)

    if helping:
        @when(lends)
        def _():
            @functools.partial(over, hold, groups)
            def _(g):
                give_back(g).wait_recv()
                finish(g, True)

    @functools.partial(over, back_lo, back_hi)
    def _(g):
        for i in range(1, steps):
            sent(flux_halo(i, g))

    if helping:
        @when(is_last)
        def _():
            over(hold, groups, lambda g: give_back(g).wait_send())


def solution(mesh):
    windows, tiles = mesh.shape["win"], mesh.shape["tile"]

    def body(state, obs, trajectory, coupling, prec):
        block = state.shape[2:]
        variables, levels, cx, cy = block
        steps = trajectory.shape[2]
        groups = levels // GROUP
        keep, hold = (groups // 2, groups - groups // 4) if windows > 3 else (groups, groups)
        slots, half = 2 * steps + 1, GROUP // 2
        flat = (variables, levels * cx, cy)
        field = (variables, groups, cx, GROUP, cy)
        anywhere = pl.BlockSpec(memory_space=pltpu.HBM)
        f32 = jnp.float32
        result = pl.pallas_call(
            functools.partial(kernel, windows, tiles, keep, hold),
            out_shape=jax.ShapeDtypeStruct(flat, f32),
            in_specs=[anywhere] * 5,
            out_specs=pl.BlockSpec(memory_space=pltpu.VMEM),
            scratch_shapes=[
                pltpu.VMEM(flat, f32),
                pltpu.VMEM(flat, f32),
                pltpu.VMEM((2 * steps, levels, cx, cy), trajectory.dtype),
                pltpu.SMEM(coupling.shape, f32),
                pltpu.SMEM(prec.shape, f32),
                pltpu.VMEM((steps + 2,) + field, f32),
                pltpu.VMEM((2 * steps, groups, cx, GROUP, cy), f32),
                pltpu.VMEM(field, f32),
                pltpu.VMEM(field, f32),
                pltpu.VMEM((steps,) + field, f32),
                pltpu.VMEM(field, f32),
                pltpu.VMEM((steps + 1, 2, groups, variables, GROUP, cy), f32),
                pltpu.VMEM((slots, 2, groups, variables, GROUP, cy), f32),
                pltpu.VMEM((slots, 2, groups, half, cy), f32),
                pltpu.VMEM((slots, 2, groups, half, cy), f32),
                pltpu.VMEM((2, groups, GROUP, cy), f32),
                pltpu.VMEM((2, groups, variables, GROUP, cy), f32),
                pltpu.VMEM((groups, GROUP, cy), f32),
                pltpu.VMEM((2, groups, GROUP, cy), f32),
                pltpu.VMEM((groups, GROUP, cy), f32),
                pltpu.SemaphoreType.DMA((groups + steps + 3,)),
                pltpu.SemaphoreType.DMA((slots, 4, groups)),
                pltpu.SemaphoreType.DMA((slots, 4, groups)),
                pltpu.SemaphoreType.DMA((2, groups)),
                pltpu.SemaphoreType.DMA((2, groups)),
                pltpu.SemaphoreType.DMA((2 + steps, groups)),
                pltpu.SemaphoreType.DMA((2 + steps, groups)),
                pltpu.SemaphoreType.DMA((3, groups)),
                pltpu.SemaphoreType.DMA((3, groups)),
                pltpu.SemaphoreType.DMA((3, groups)),
                pltpu.SemaphoreType.DMA((3, groups)),
            ],
            compiler_params=pltpu.CompilerParams(
                collective_id=0, has_side_effects=True, vmem_limit_bytes=48 * 2**20),
        )(*[pltpu.with_memory_space_constraint(x, pltpu.HBM) for x in (
            state.reshape(flat), obs.reshape(flat),
            trajectory.reshape((2 * steps, levels, cx, cy)), coupling, prec)])
        return result.reshape((1, 1) + block)

    spec = P("win", "tile", None, None, None, None)
    return jax.shard_map(
        body, mesh=mesh,
        in_specs=(spec, spec, P("win", "tile", None, None, None, None, None), P(), P()),
        out_specs=spec, check_vma=False)
```

```python
import functools

import jax
import jax.numpy as jnp
from jax import lax
from jax.experimental import pallas as pl
from jax.experimental.pallas import tpu as pltpu
from jax.sharding import PartitionSpec as P

TY = 4
GROUP = 8

smooth_weight = 0.2


def kernel(windows, tiles, keep, hold, state, obs, winds, coupling, prec, out,
           nat, onat, wnat, cs, ps, fld, wr, arrived, wgt, gf, ret, xs, xr, ys, yr, yp, xe, ye, xw, yw,
           load, hsend, hrecv, wsend, wrecv, msend, mrecv, esend, erecv, fsend, frecv):
    steps, groups, cx, cy = wr.shape[0] // 2, wr.shape[1], wr.shape[2], wr.shape[4]
    variables = fld.shape[1]
    span = GROUP * cx
    end = windows - 1
    gap, back0 = steps, steps + 1
    half = GROUP // 2
    helping = keep < groups
    k = lax.axis_index("win")
    t = lax.axis_index("tile")
    before_x, after_x = lax.rem(t + tiles - TY, tiles), lax.rem(t + TY, tiles)
    before_y, after_y = lax.rem(t + tiles - 1, tiles), lax.rem(t + 1, tiles)
    around = (before_x, after_x, before_y, after_y)
    lender = end - 2
    is_first, is_last, lends = k == 0, k == end, k == lender
    lo, hi = jnp.where(is_last, keep, 0), jnp.where(lends, keep, groups)
    back_lo, back_hi = jnp.where(is_last, hold, 0), jnp.where(lends, hold, groups)
    sel = jnp.where(is_last, 1, 0)
    nxt = jnp.where(is_last, lender + 1, k + 1)

    def when(cond):
        return pl.when(cond)

    def part(g):
        return pl.ds(pl.multiple_of(g * span, span), span)

    def state_in(g):
        return pltpu.make_async_copy(state.at[:, part(g)], nat.at[:, part(g)], load.at[g])

    def winds_in(n):
        return pltpu.make_async_copy(winds.at[pl.ds(2 * n, 2)], wnat.at[pl.ds(2 * n, 2)], load.at[groups + n])

    obs_in = pltpu.make_async_copy(obs, onat, load.at[groups + steps])
    prec_in = pltpu.make_async_copy(prec, ps, load.at[groups + steps + 1])
    coupling_in = pltpu.make_async_copy(coupling, cs, load.at[groups + steps + 2])

    order = tuple(reversed(range(groups)))
    for g in order:
        state_in(g).start()
    coupling_in.start()

    @when(~is_last)
    def _():
        for n in range(steps):
            winds_in(n).start()
    prec_in.start()
    obs_in.start()

    barrier = pltpu.get_barrier_semaphore()

    def greet(win):
        pl.semaphore_signal(barrier, inc=1, device_id={"win": win})

    for other in around:
        pl.semaphore_signal(barrier, inc=1, device_id={"tile": other})

    @when(k < end)
    def _():
        greet(k + 1)

    @when(k > 0)
    def _():
        greet(k - 1)

    met = len(around) + jnp.where(k < end, 1, 0) + jnp.where(k > 0, 1, 0)
    if helping:
        @when(lends)
        def _():
            greet(end)

        @when(is_last)
        def _():
            greet(lender)
        met = met + jnp.where(lends | is_last, 1, 0)

    shape = (GROUP, cy)
    lane = lax.broadcasted_iota(jnp.int32, shape, 1)
    level = lax.broadcasted_iota(jnp.int32, shape, 0)
    pair, odd = lane // 2, lane % 2 == 1
    at_start, at_end = lane == 0, lane == cy - 1

    def halo(slot, g, win, low, high):
        made = []
        for side, to in enumerate((before_y, after_y)):
            made.append(pltpu.make_async_remote_copy(
                src_ref=ys.at[slot, side, g], dst_ref=yr.at[slot, side, g],
                send_sem=hsend.at[slot, side, g], recv_sem=hrecv.at[slot, side, g],
                device_id={"win": win, "tile": to}))
        for side, (to, rows) in enumerate(((before_x, low), (after_x, high))):
            made.append(pltpu.make_async_remote_copy(
                src_ref=rows, dst_ref=xr.at[slot, side, g],
                send_sem=hsend.at[slot, 2 + side, g], recv_sem=hrecv.at[slot, 2 + side, g],
                device_id={"win": win, "tile": to}))
        return made

    def field_halo(slot, g, index):
        return halo(slot, g, k, fld.at[index, :, g, 0], fld.at[index, :, g, cx - 1])

    def gap_halo(g):
        return halo(gap, g, nxt, xs.at[0, 0, g], xs.at[0, 1, g])

    def weighted_halo(g):
        return halo(back0, g, source(g, hold), xs.at[steps, 0, g], xs.at[steps, 1, g])

    def flux_halo(i, g):
        return halo(back0 + i, g, k, xs.at[i, 0, g], xs.at[i, 1, g])

    def receive(slot, g):
        for copy in halo(slot, g, k, xr.at[slot, 0, g], xr.at[slot, 1, g]):
            copy.wait_recv()

    def source(g, bound):
        return jnp.where((k == lender + 1) & (g >= bound), end, k - 1)

    def local_edges(pieces, sends, arrives, g, win):
        return [pltpu.make_async_remote_copy(
            src_ref=src, dst_ref=dst, send_sem=sends.at[i, g], recv_sem=arrives.at[i, g], device_id={"win": win})
            for i, (src, dst) in enumerate(pieces)]

    def state_edges(g):
        return local_edges((
            (fld.at[0, :, g, 0], xe.at[0, g]), (fld.at[0, :, g, cx - 1], xe.at[1, g]), (yp.at[0, g], ye.at[g]),
        ), esend, erecv, g, source(g, keep))

    def wind_edges(g):
        n = 2 * steps - 2
        return local_edges((
            (wr.at[n, g, 0], xw.at[0, g]), (wr.at[n, g, cx - 1], xw.at[1, g]), (yp.at[1, g], yw.at[g]),
        ), fsend, frecv, g, k + 1)

    def onward(g):
        return pltpu.make_async_remote_copy(
            src_ref=fld.at[steps + 1, :, g], dst_ref=arrived.at[:, g],
            send_sem=wsend.at[0, g], recv_sem=wrecv.at[0, g], device_id={"win": nxt})

    def back(g):
        return pltpu.make_async_remote_copy(
            src_ref=wgt.at[:, g], dst_ref=gf.at[0, :, g],
            send_sem=wsend.at[1, g], recv_sem=wrecv.at[1, g], device_id={"win": source(g, hold)})

    def lend_state(g):
        return pltpu.make_async_remote_copy(
            src_ref=fld.at[0, :, g], dst_ref=fld.at[1, :, g],
            send_sem=msend.at[0, g], recv_sem=mrecv.at[0, g], device_id={"win": end})

    def lend_winds(n, g):
        return pltpu.make_async_remote_copy(
            src_ref=wr.at[pl.ds(2 * n, 2), g], dst_ref=wr.at[pl.ds(2 * n, 2), g],
            send_sem=msend.at[2 + n, g], recv_sem=mrecv.at[2 + n, g], device_id={"win": end})

    def give_back(g):
        return pltpu.make_async_remote_copy(
            src_ref=ret.at[:, g], dst_ref=ret.at[:, g],
            send_sem=msend.at[1, g], recv_sem=mrecv.at[1, g], device_id={"win": lender})

    def place(v, r):
        return v * cx + r

    def pack(packed, value, v, r):
        p = place(v, r)
        return jnp.where(pair == p, pltpu.roll(value, 2 * p + 1, 1), packed)

    def fold(slot, g, packed):
        upper = pltpu.roll(pltpu.roll(packed, half, 0), 1, 1)
        ys[slot, 0, g] = jnp.where(odd, packed, upper)[:half]
        ys[slot, 1, g] = jnp.where(odd, upper, packed)[:half]

    def unfold(slot, g):
        north, south = [jnp.concatenate([yr[slot, side, g]] * 2, axis=0) for side in range(2)]
        north = jnp.where(level < half, north, pltpu.roll(north, cy - 1, 1))
        south = jnp.where(level < half, pltpu.roll(south, 2, 1), pltpu.roll(south, 1, 1))
        return jnp.where(odd, north, south)

    def sides(value, rim, v, r):
        edge_pair = pltpu.roll(rim, cy - 2 - 2 * place(v, r), 1)
        north = jnp.where(at_end, edge_pair, pltpu.roll(value, cy - 1, 1))
        south = jnp.where(at_start, edge_pair, pltpu.roll(value, 1, 1))
        return north, south

    def every(f):
        for v in range(variables):
            f(v)

    def rows_of(g, r):
        return pl.ds(g * span + r, GROUP, stride=cx)

    def convert_state(g):
        for v in range(variables):
            for r in range(cx):
                fld[0, v, g, r] = nat[v, rows_of(g, r), :]

    def pack_state(g, index):
        packed = jnp.zeros(shape, jnp.float32)
        for v in range(variables):
            for r in range(cx):
                packed = pack(packed, fld[index, v, g, r], v, r)
        return packed

    def start(copies):
        for copy in copies:
            copy.start()

    def over(a, b, f):
        lax.fori_loop(a, b, lambda i, c: (f(a + b - 1 - i), c)[1], 0)

    for g in order:
        state_in(g).wait()
        convert_state(g)
        packed = pack_state(g, 0)
        fold(0, g, packed)
        yp[0, g] = packed
    pl.semaphore_wait(barrier, met)
    for g in order:
        if g >= keep:
            @when(lends)
            def _():
                lend_state(g).start()

    for part_of in (slice(0, 2), slice(2, 4)):
        for g in order:
            @when((k < end) & (g < hi))
            def _():
                start(field_halo(0, g, 0)[part_of])

    @when(k > 0)
    def _():
        over(0, groups, lambda g: start(state_edges(g)))

    def convert_winds(n, g):
        for way in range(2):
            for j in range(GROUP):
                tile = wnat[2 * n + way, g * GROUP + j].astype(jnp.float32)
                for r in range(cx):
                    wr[2 * n + way, g, r, pl.ds(j, 1), :] = tile[r:r + 1]

    @when(k < end)
    def _():
        for n in range(steps):
            winds_in(n).wait()

            def one(i, n=n):
                g = lax.rem(i + keep, groups)
                convert_winds(n, g)
                if helping:
                    @when(lends & (g >= keep))
                    def _():
                        lend_winds(n, g).start()
            over(0, groups, one)

        @functools.partial(over, 0, groups)
        def _(g):
            packed = jnp.zeros(shape, jnp.float32)
            for r in range(cx):
                packed = pack(packed, wr[2 * steps - 1, g, r], 0, r)
            total = packed
            for v in range(1, variables):
                total = total + pltpu.roll(packed, 2 * place(v, 0), 1)
            yp[1, g] = total
            start(wind_edges(g))

    coupling_in.wait()

    if helping:
        @when(is_last)
        def _():
            @functools.partial(over, keep, groups)
            def _(g):
                lend_state(g).wait_recv()
                fold(0, g, pack_state(g, 1))
                start(field_halo(0, g, 1))

    def forward(n, g, final):
        if helping:
            @when(is_last)
            def _():
                lend_winds(n, g).wait_recv()
        receive(n, g)
        index = jnp.where(n == 0, sel, n + 1)
        rim = unfold(n, g)
        if final:
            for copy in state_edges(g):
                copy.wait_recv()

        def row(r):
            if r < 0:
                return [xr[n, 1, g, v] for v in range(variables)]
            if r == cx:
                return [xr[n, 0, g, v] for v in range(variables)]
            return [fld[index, v, g, r] for v in range(variables)]

        west, here = row(-1), row(0)
        packed = jnp.zeros(shape, jnp.float32)
        for r in range(cx):
            east = row(r + 1)
            u, w = wr[2 * n, g, r], wr[2 * n + 1, g, r]
            for v in range(variables):
                north, south = sides(here[v], rim, v, r)
                total = here[v] + u * (east[v] - west[v]) + w * (north - south)
                for b in range(variables):
                    total = total + cs[v, b] * here[b]
                fld[n + 2, v, g, r] = total
                if final and r == 0:
                    xs[0, 0, g, v] = xe[0, g, v] - total
                if final and r == cx - 1:
                    xs[0, 1, g, v] = xe[1, g, v] - total
                packed = pack(packed, total, v, r)
            west, here = here, east
        if final:
            fold(gap, g, ye[g] - packed)
            start(gap_halo(g))
            onward(g).start()
        else:
            fold(n + 1, g, packed)
            start(field_halo(n + 1, g, n + 2))

    def early_steps(n):
        over(lo, hi, lambda g: forward(n, g, False))

    lax.fori_loop(0, steps - 1, lambda n, c: (early_steps(n), c)[1], 0)
    over(lo, hi, lambda g: forward(steps - 1, g, True))

    prec_in.wait()

    def stencil(g, row, rim, keeps):
        scale = []
        for v in range(variables):
            s = jnp.zeros(shape, jnp.float32)
            for j in range(GROUP):
                s = jnp.where(level == j, ps[v, g * GROUP + j], s)
            scale.append(s)
        west, here = row(-1), row(0)
        packed = jnp.zeros(shape, jnp.float32)
        for r in range(cx):
            east = row(r + 1)
            for v in range(variables):
                north, south = sides(here[v], rim, v, r)
                smooth = (1.0 + 4.0 * smooth_weight) * here[v] - smooth_weight * (
                    east[v] + west[v] + north + south)
                total = scale[v] * smooth
                wgt[v, g, r] = total
                if keeps:
                    packed = pack(packed, total, v, r)
                if keeps and r == 0:
                    xs[steps, 0, g, v] = xw[0, g] * total
                if keeps and r == cx - 1:
                    xs[steps, 1, g, v] = xw[1, g] * total
            west, here = here, east
        return packed

    def start_window(g):
        def row(r):
            if r < 0:
                return [xr[0, 1, g, v] for v in range(variables)]
            if r == cx:
                return [xr[0, 0, g, v] for v in range(variables)]
            return [fld[0, v, g, r] for v in range(variables)]
        stencil(g, row, unfold(0, g), False)

    def mismatch(g):
        receive(gap, g)
        onward(g).wait_recv()
        for copy in wind_edges(g):
            copy.wait_recv()

        def row(r):
            if r < 0:
                return [xr[gap, 1, g, v] for v in range(variables)]
            if r == cx:
                return [xr[gap, 0, g, v] for v in range(variables)]
            return [fld[0, v, g, r] - arrived[v, g, r] for v in range(variables)]
        fold(back0, g, yw[g] * stencil(g, row, unfold(gap, g), True))
        start(weighted_halo(g))
        back(g).start()

    @when(k > 0)
    def _():
        over(0, groups, lambda i: mismatch(jnp.where((k == 2) & (i < hold), lax.rem(i + keep, hold), i)))

    @when(is_first)
    def _():
        over(0, groups, start_window)

    def backward(i, g):
        n = steps - 1 - i
        slot = back0 + i
        first, final = i == 0, i == steps - 1
        if first:
            back(g).wait_recv()
        receive(slot, g)
        rim = unfold(slot, g)

        def row(r):
            if r < 0:
                return None, [xr[slot, 1, g, v] for v in range(variables)]
            if r == cx:
                return None, [xr[slot, 0, g, v] for v in range(variables)]
            u = wr[2 * n, g, r]
            values = [gf[i, v, g, r] for v in range(variables)]
            return values, [u * value for value in values]

        (_, west), (values, here) = row(-1), row(0)
        packed = jnp.zeros(shape, jnp.float32)
        for r in range(cx):
            values_east, east = row(r + 1)
            w = wr[2 * n + 1, g, r]
            if not final:
                u_next, w_next = wr[2 * n - 2, g, r], wr[2 * n - 1, g, r]
            for v in range(variables):
                north, south = sides(w * values[v], rim, v, r)
                total = values[v] + (west[v] - east[v]) + (south - north)
                for b in range(variables):
                    total = total + cs[b, v] * values[b]
                if final:
                    rows = rows_of(g, r)
                    ret[v, g, r] = total
                    out[v, rows, :] = wgt[v, g, r] + onat[v, rows, :] * fld[0, v, g, r] - total
                    continue
                gf[i + 1, v, g, r] = total
                if r == 0:
                    xs[i + 1, 0, g, v] = u_next * total
                if r == cx - 1:
                    xs[i + 1, 1, g, v] = u_next * total
                packed = pack(packed, w_next * total, v, r)
            west, values, here = here, values_east, east
        if not final:
            fold(slot + 1, g, packed)
            start(flux_halo(i + 1, g))

    for i in range(steps - 1):
        over(back_lo, back_hi, lambda j, i=i: backward(i, jnp.where(k == 1, lax.rem(j + keep, hold), j)))

    def sent(copies):
        for copy in copies:
            copy.wait_send()

    @functools.partial(over, lo, hi)
    def _(g):
        for n in range(steps):
            sent(field_halo(n, g, 0))
        sent(gap_halo(g))
        onward(g).wait_send()

    @when(k > 0)
    def _():
        @functools.partial(over, 0, groups)
        def _(g):
            sent(weighted_halo(g))
            sent(state_edges(g))
            back(g).wait_send()

    @when(k < end)
    def _():
        over(0, groups, lambda g: sent(wind_edges(g)))

    if helping:
        @when(lends)
        def _():
            @functools.partial(over, keep, groups)
            def _(g):
                lend_state(g).wait_send()
                for n in range(steps):
                    lend_winds(n, g).wait_send()

    obs_in.wait()

    def finish(g, has_next):
        for v in range(variables):
            for r in range(cx):
                rows = rows_of(g, r)
                own = wgt[v, g, r] + onat[v, rows, :] * fld[0, v, g, r]
                out[v, rows, :] = own - ret[v, g, r] if has_next else own

    @functools.partial(over, back_lo, back_hi)
    def _(j):
        g = jnp.where(k == 1, lax.rem(j + keep, hold), j)
        backward(steps - 1, g)

        if helping:
            @when(is_last)
            def _():
                give_back(g).start()

    @when(is_last)
    def _():
        @functools.partial(over, 0, groups)
        def _(g):
            finish(g, False)

    if helping:
        @when(lends)
        def _():
            @functools.partial(over, hold, groups)
            def _(g):
                give_back(g).wait_recv()
                finish(g, True)

    @functools.partial(over, back_lo, back_hi)
    def _(g):
        for i in range(1, steps):
            sent(flux_halo(i, g))

    if helping:
        @when(is_last)
        def _():
            over(hold, groups, lambda g: give_back(g).wait_send())


def solution(mesh):
    windows, tiles = mesh.shape["win"], mesh.shape["tile"]

    def body(state, obs, trajectory, coupling, prec):
        block = state.shape[2:]
        variables, levels, cx, cy = block
        steps = trajectory.shape[2]
        groups = levels // GROUP
        keep, hold = (groups // 2, groups - groups // 4) if windows > 3 else (groups, groups)
        slots, half = 2 * steps + 1, GROUP // 2
        flat = (variables, levels * cx, cy)
        field = (variables, groups, cx, GROUP, cy)
        anywhere = pl.BlockSpec(memory_space=pltpu.HBM)
        f32 = jnp.float32
        result = pl.pallas_call(
            functools.partial(kernel, windows, tiles, keep, hold),
            out_shape=jax.ShapeDtypeStruct(flat, f32),
            in_specs=[anywhere] * 5,
            out_specs=pl.BlockSpec(memory_space=pltpu.VMEM),
            scratch_shapes=[
                pltpu.VMEM(flat, f32),
                pltpu.VMEM(flat, f32),
                pltpu.VMEM((2 * steps, levels, cx, cy), trajectory.dtype),
                pltpu.SMEM(coupling.shape, f32),
                pltpu.SMEM(prec.shape, f32),
                pltpu.VMEM((steps + 2,) + field, f32),
                pltpu.VMEM((2 * steps, groups, cx, GROUP, cy), f32),
                pltpu.VMEM(field, f32),
                pltpu.VMEM(field, f32),
                pltpu.VMEM((steps,) + field, f32),
                pltpu.VMEM(field, f32),
                pltpu.VMEM((steps + 1, 2, groups, variables, GROUP, cy), f32),
                pltpu.VMEM((slots, 2, groups, variables, GROUP, cy), f32),
                pltpu.VMEM((slots, 2, groups, half, cy), f32),
                pltpu.VMEM((slots, 2, groups, half, cy), f32),
                pltpu.VMEM((2, groups, GROUP, cy), f32),
                pltpu.VMEM((2, groups, variables, GROUP, cy), f32),
                pltpu.VMEM((groups, GROUP, cy), f32),
                pltpu.VMEM((2, groups, GROUP, cy), f32),
                pltpu.VMEM((groups, GROUP, cy), f32),
                pltpu.SemaphoreType.DMA((groups + steps + 3,)),
                pltpu.SemaphoreType.DMA((slots, 4, groups)),
                pltpu.SemaphoreType.DMA((slots, 4, groups)),
                pltpu.SemaphoreType.DMA((2, groups)),
                pltpu.SemaphoreType.DMA((2, groups)),
                pltpu.SemaphoreType.DMA((2 + steps, groups)),
                pltpu.SemaphoreType.DMA((2 + steps, groups)),
                pltpu.SemaphoreType.DMA((3, groups)),
                pltpu.SemaphoreType.DMA((3, groups)),
                pltpu.SemaphoreType.DMA((3, groups)),
                pltpu.SemaphoreType.DMA((3, groups)),
            ],
            compiler_params=pltpu.CompilerParams(
                collective_id=0, has_side_effects=True, vmem_limit_bytes=48 * 2**20),
        )(*[pltpu.with_memory_space_constraint(x, pltpu.HBM) for x in (
            state.reshape(flat), obs.reshape(flat),
            trajectory.reshape((2 * steps, levels, cx, cy)), coupling, prec)])
        return result.reshape((1, 1) + block)

    spec = P("win", "tile", None, None, None, None)
    return jax.shard_map(
        body, mesh=mesh,
        in_specs=(spec, spec, P("win", "tile", None, None, None, None, None), P(), P()),
        out_specs=spec, check_vma=False)
```
